256 devices in a mesh: variant: 8 (over y, x_lo), mp: 32 (over x_hi, z, core).
Axes of the slice: x: 4 (x_hi: 2, x_lo: 2; x = x_hi * 2 + x_lo), y: 4, z: 8, core: 2. Of those that a mesh axis runs over, the one named last changes fastest.
Arguments:
- positions: bfloat16 [131072, 1024], P(('variant', 'mp')), may hold values from -6 to 6
- game_counts: int32 [256], P(('variant', 'mp')), may hold values from 384 to 512
- block_variant: int32 [1024], P(('variant', 'mp')), may hold values from 0 to 7, as said below
- norm_gain: float32 [8, 1024], P('variant'), may hold values from 0.25 to 1.75
- up_weight: bfloat16 [8, 1024, 2048], P('variant', 'mp'), may hold values from -0.1875 to 0.1875
- down_weight: bfloat16 [8, 2048, 1024], P('variant', 'mp'), may hold values from -0.125 to 0.125
- final_gain: float32 [8, 1024], P('variant'), may hold values from 0.25 to 1.75
- value_weight: float32 [8, 1024], P('variant'), may hold values from -0.1875 to 0.1875
- policy_weight: bfloat16 [1024, 2336], P(('variant', 'mp')), may hold values from -0.1875 to 0.1875
Outputs:
- policy: bfloat16 [131072, 2336], P(('variant', 'mp'))
- value: float32 [131072], P(('variant', 'mp'))
The draws below stay inside these ranges and needn't reach their ends.
Inputs may be any that keep to these rules, and one draw needn't show every extreme that they name: `block_variant`: the 4 blocks of one device name 4 different variants.
All inputs are finite; a program needn't handle non-finite values.
Results may differ from the reference program's by a relative error of at most 0.0056.
Values may be sent and summed in bfloat16 or wider, within the bound.
A program may use at most 128 MiB of HBM per device.

```python
import jax
import jax.numpy as jnp
from jax import lax

D = 1024
FFW = 2048
POLICY = 2336
BLOCK = 128
BLOCKS_DEV = 4
VARIANTS = 8
DEVS = 256
GAMES_DEV = 512
GAMES = 131072
BLOCKS = 1024


def draw_block_variant(key, part):
    devices = BLOCKS // BLOCKS_DEV
    labels = jax.random.permutation(jax.random.fold_in(key, 11), VARIANTS).astype(jnp.int32)
    jitter = jax.random.randint(jax.random.fold_in(key, 12), (devices, VARIANTS), 0, 1000)
    preference = (VARIANTS - 1 - jnp.arange(VARIANTS, dtype=jnp.int32)) * 120
    ranking = (jitter + preference[None, :]) * VARIANTS + jnp.arange(VARIANTS, dtype=jnp.int32)[None, :]
    chosen = lax.top_k(ranking, BLOCKS_DEV)[1].astype(jnp.int32)
    shuffle_keys = jax.random.randint(jax.random.fold_in(key, 13), (devices, BLOCKS_DEV), 0, 1000) * BLOCKS_DEV
    shuffle_keys = shuffle_keys + jnp.arange(BLOCKS_DEV, dtype=jnp.int32)[None, :]
    shuffle = jnp.argsort(shuffle_keys, axis=1, stable=True)
    chosen = jnp.take_along_axis(chosen, shuffle, axis=1)
    return labels[chosen].reshape(BLOCKS).astype(jnp.int32)


def touch_ends(result, key, smallest, largest):
    longest = result.shape.index(max(result.shape))
    spots = []
    for shift in (0, 1):
        where = [jax.random.randint(jax.random.fold_in(key, axis), (), 0, length) for axis, length in enumerate(result.shape)]
        where[longest] = (where[longest] + shift) % result.shape[longest]
        spots.append(tuple(where))
    return result.at[spots[0]].set(smallest).at[spots[1]].set(largest)


def levels(key, dims, cuts, smallest, high):
    level, own = 1.0, jax.random.fold_in(key, 6)
    for position, shards_of in cuts:
        steps = jnp.exp(jax.random.uniform(jax.random.fold_in(own, position), (shards_of,), jnp.float32, smallest / len(cuts), high / len(cuts)))
        level = level * jnp.repeat(steps, dims[position] // shards_of).reshape([-1 if axis == position else 1 for axis in range(len(dims))])
    return level


def noise(rng, extent, width, most, cuts=(), kind=jnp.bfloat16):
    result = jax.random.normal(rng, extent, jnp.float32) * width
    if len(cuts) > 0:
        result = levels(rng, extent, cuts, -0.22, 0.18) * result
    return jnp.clip(result, min=-most, max=most).astype(kind)


def setup_inputs(seed: int = 0) -> dict:
    streams_of = jax.random.split(jax.random.key(seed), 10)
    return {
        "positions": noise(streams_of[0], (GAMES, D), 1.0, 6.0, ((0, 256),)),
        "game_counts": touch_ends(jax.random.randint(streams_of[1], (DEVS,), GAMES_DEV * 3 // 4, GAMES_DEV + 1), jax.random.fold_in(streams_of[1], 1), GAMES_DEV * 3 // 4, GAMES_DEV).astype(jnp.int32),
        "block_variant": draw_block_variant(jax.random.fold_in(streams_of[9], 71), 0),
        "norm_gain": jnp.clip(1.0 + 0.15 * jax.random.normal(streams_of[3], (VARIANTS, D), jnp.float32), 0.25, 1.75),
        "up_weight": noise(streams_of[4], (VARIANTS, D, FFW), D ** -0.5, 0.1875, ((0, 8), (1, 32))),
        "down_weight": noise(streams_of[5], (VARIANTS, FFW, D), FFW ** -0.5, 0.125, ((0, 8), (1, 32))),
        "final_gain": jnp.clip(1.0 + 0.15 * jax.random.normal(streams_of[6], (VARIANTS, D), jnp.float32), 0.25, 1.75),
        "value_weight": noise(streams_of[7], (VARIANTS, D), D ** -0.5, 0.1875, ((0, 8),), jnp.float32),
        "policy_weight": noise(streams_of[8], (D, POLICY), D ** -0.5, 0.1875, ((0, 256),)),
    }


def rms_scale(values, scale_gain):
    mean_square = lax.optimization_barrier(jnp.mean(values * values, axis=-1, keepdims=True))
    return values * lax.rsqrt(mean_square + 1e-06) * scale_gain

def evaluate(block_rows, variant, norm_gain, up_weight, down_weight, final_gain, value_weight, policy_weight):
    values = block_rows.astype(jnp.float32)
    normed = rms_scale(values, norm_gain[variant]).astype(jnp.bfloat16)
    upward = jnp.dot(normed, up_weight[variant], preferred_element_type=jnp.float32)
    active = jax.nn.gelu(upward, approximate=True).astype(jnp.bfloat16)
    downward = jnp.dot(active, down_weight[variant], preferred_element_type=jnp.float32)
    hidden = rms_scale(values + downward, final_gain[variant])
    estimate = jnp.tanh(lax.optimization_barrier(jnp.sum(hidden * value_weight[variant], axis=-1)))
    logits = jnp.dot(hidden.astype(jnp.bfloat16), policy_weight, preferred_element_type=jnp.float32).astype(jnp.bfloat16)
    return (logits, estimate)

def reference(positions, game_counts, block_variant, norm_gain, up_weight, down_weight, final_gain, value_weight, policy_weight):
    blocks = positions.reshape(BLOCKS, BLOCK, D)

    def one_block(slot_entry):
        return evaluate(slot_entry[0], slot_entry[1], norm_gain, up_weight, down_weight, final_gain, value_weight, policy_weight)
    logits, estimate = lax.map(one_block, (blocks, block_variant))
    logits = logits.reshape(GAMES, POLICY)
    estimate = estimate.reshape(GAMES)
    row_ids = jnp.arange(GAMES, dtype=jnp.int32)
    owner_ids = row_ids // GAMES_DEV
    row_live = row_ids % GAMES_DEV < game_counts[owner_ids]
    policy = jnp.where(row_live[:, None], logits, jnp.zeros((), jnp.bfloat16))
    value = jnp.where(row_live, estimate, jnp.zeros((), jnp.float32))
    return (policy, value)
```

```python
import functools

import jax
import jax.numpy as jnp
from jax import lax
from jax.experimental import pallas as pl
from jax.experimental.pallas import tpu as pltpu
from jax.sharding import PartitionSpec as P

MESH = pl.DeviceIdType.MESH
BLOCK = 128
EPS = 1e-06
XLO, XHI, CORES = 2, 2, 2
GROUP = 2


def rms_scale(values, gain):
    mean_square = jnp.mean(values * values, axis=-1, keepdims=True)
    return values * lax.rsqrt(mean_square + EPS) * gain


def remote(src, dst, send_sem, recv_sem, device):
    return pltpu.make_async_remote_copy(
        src_ref=src, dst_ref=dst, send_sem=send_sem, recv_sem=recv_sem, device_id=device, device_id_type=MESH
    )


def exchange_kernel(
    variants,
    members,
    bv_ref,
    pos_ref,
    up_ref,
    down_ref,
    ng_ref,
    fg_ref,
    vw_ref,
    hid_out,
    val_out,
    outgoing,
    incoming,
    normed,
    active,
    up_all,
    down_all,
    hidden,
    returned,
    estimate,
    estimate_back,
    ring_recv,
    plus_send,
    minus_send,
    core_send,
    half_send,
    slot_send,
    slot_recv,
    back_send,
    back_recv,
    value_send,
    value_recv,
):
    ys, zs = variants // XLO, members // (XHI * CORES)
    v, m = lax.axis_index("variant"), lax.axis_index("mp")
    y, xl = lax.div(v, XLO), lax.rem(v, XLO)
    xh, z, core = lax.div(m, zs * CORES), lax.rem(lax.div(m, CORES), zs), lax.rem(m, CORES)

    def member(xr, dz, cr):
        return (lax.rem(xh + xr, XHI) * zs + lax.rem(z + dz, zs)) * CORES + lax.rem(core + cr, CORES)

    def peer(dy, dx):
        return lax.rem(y + dy, ys) * XLO + lax.rem(xl + dx, XLO)

    z_plus, z_minus = (v, member(0, 1, 0)), (v, member(0, zs - 1, 0))
    sibling, half = (v, member(0, 0, 1)), (v, member(1, 0, 0))
    order = sorted(
        ((dy, dx) for dy in range(ys) for dx in range(XLO)), key=lambda r: (-min(r[0], ys - r[0]), -r[1])
    )
    to_peer = [(peer(dy, dx), m) for dy, dx in order]
    from_peer = [(peer(ys - dy, XLO - dx), m) for dy, dx in order]
    slots = len(order)
    local = slots - 1

    barrier = pltpu.get_barrier_semaphore()
    greeted = [z_plus, z_minus, sibling, half, *to_peer[:local]]
    for device in greeted:
        pl.semaphore_signal(barrier, inc=1, device_id=device, device_id_type=MESH)
    pl.semaphore_wait(barrier, len(greeted))

    shards, wholes = (up_ref, down_ref), (up_all, down_all)

    def rows(kind, xr, dist, cr):
        depth = shards[kind].shape[0]
        owner = member(xr, zs - dist, cr)
        return wholes[kind].at[pl.ds(pl.multiple_of(owner * depth, depth), depth)]

    def source(kind, xr, dist):
        return shards[kind] if (xr, dist) == (0, 0) else rows(kind, xr, dist, 0)

    sent = []

    def send(copy):
        copy.start()
        sent.append(copy)

    def send_half(kind):
        send(remote(shards[kind], rows(kind, 0, 0, 0), half_send.at[kind], ring_recv.at[kind, 1, 0, 0], half))

    def send_plus(kind, xr, dist):
        send(
            remote(
                source(kind, xr, dist),
                rows(kind, xr, dist, 0),
                plus_send.at[kind, xr, dist],
                ring_recv.at[kind, xr, dist + 1, 0],
                z_plus,
            )
        )

    def send_minus(kind, xr, dist):
        send(
            remote(
                source(kind, xr, dist),
                rows(kind, xr, dist, 0),
                minus_send.at[kind, xr, dist],
                ring_recv.at[kind, xr, (dist - 1) % zs, 0],
                z_minus,
            )
        )

    def send_core(kind, xr, dist):
        send(
            remote(
                source(kind, xr, dist),
                rows(kind, xr, dist, 0),
                core_send.at[kind, xr, dist],
                ring_recv.at[kind, xr, dist, 1],
                sibling,
            )
        )

    def arrived(kind, xr, dist, cr):
        ref = rows(kind, xr, dist, cr)
        remote(ref, ref, core_send.at[kind, xr, dist], ring_recv.at[kind, xr, dist, cr], sibling).wait_recv()

    plus = (zs // 2, zs - 1 - zs // 2)
    minus = (zs - 1 - zs // 2, zs // 2)
    steps = zs // 2

    def begin_own(kind):
        send_plus(kind, 0, 0)
        send_minus(kind, 0, 0)
        send_core(kind, 0, 0)

    def begin_half(kind):
        arrived(kind, 1, 0, 0)
        send_plus(kind, 1, 0)
        send_minus(kind, 1, 0)
        send_core(kind, 1, 0)

    def ring_step(kind, step):
        for xr in range(XHI):
            if step <= plus[kind]:
                arrived(kind, xr, step, 0)
                if step < plus[kind]:
                    send_plus(kind, xr, step)
                send_core(kind, xr, step)
            if step <= minus[kind]:
                arrived(kind, xr, zs - step, 0)
                if step < minus[kind]:
                    send_minus(kind, xr, zs - step)
                send_core(kind, xr, zs - step)

    send_half(0)
    begin_own(0)
    send_half(1)

    def fill(k):
        wanted = to_peer[k][0]
        block = pos_ref[0:BLOCK, :]
        for b in range(1, bv_ref.shape[0]):
            block = jnp.where(bv_ref[b] == wanted, pos_ref[b * BLOCK : (b + 1) * BLOCK, :], block)
        if k == local:
            incoming[k] = block
        else:
            outgoing[k] = block

    def dispatch(k):
        send(remote(outgoing.at[k], incoming.at[k], slot_send.at[k], slot_recv.at[k], to_peer[k]))

    fill(0)
    for k in range(1, slots):
        fill(k)
        dispatch(k - 1)

    for kind in range(2):
        depth = shards[kind].shape[0]
        wholes[kind][pl.ds(pl.multiple_of(m * depth, depth), depth), :] = shards[kind][...]

    begin_half(0)
    for step in range(1, steps):
        ring_step(0, step)
    begin_own(1)
    begin_half(1)
    ring_step(0, steps)
    for step in range(1, steps):
        ring_step(1, step)

    for k in range(slots):
        if k != local:
            remote(outgoing.at[k], incoming.at[k], slot_send.at[k], slot_recv.at[k], to_peer[k]).wait_recv()
        normed[pl.ds(k * BLOCK, BLOCK), :] = rms_scale(incoming[k].astype(jnp.float32), ng_ref[...]).astype(
            jnp.bfloat16
        )
    for xr in range(XHI):
        for dist in range(zs):
            arrived(0, xr, dist, 1)

    total_rows = normed.shape[0]
    part_rows = total_rows // 2
    width = 256
    tiles = up_all.shape[1] // width

    def up_tiles(first, last):
        def one(i, carry):
            col = pl.multiple_of(lax.div(i, 2) * width, width)
            row = pl.multiple_of(lax.rem(i, 2) * part_rows, part_rows)
            upward = jnp.dot(
                normed[pl.ds(row, part_rows), :],
                up_all[:, pl.ds(col, width)],
                preferred_element_type=jnp.float32,
            )
            active[pl.ds(row, part_rows), pl.ds(col, width)] = jax.nn.gelu(upward, approximate=True).astype(
                jnp.bfloat16
            )
            return carry

        lax.fori_loop(2 * first, 2 * last, one, 0)

    up_tiles(0, tiles // 2)
    ring_step(1, steps)
    up_tiles(tiles // 2, tiles)
    for xr in range(XHI):
        for dist in range(zs):
            arrived(1, xr, dist, 1)

    def give_back(k):
        send(remote(hidden.at[k], returned.at[k], back_send.at[k], back_recv.at[k], from_peer[k]))
        send(remote(estimate.at[k], estimate_back.at[k], value_send.at[k], value_recv.at[k], from_peer[k]))

    for first in range(0, slots, GROUP):
        downward = jnp.dot(
            active[pl.ds(first * BLOCK, GROUP * BLOCK), :], down_all[...], preferred_element_type=jnp.float32
        )
        for k in range(first, first + GROUP):
            part = downward[(k - first) * BLOCK : (k - first + 1) * BLOCK]
            final = rms_scale(incoming[k].astype(jnp.float32) + part, fg_ref[...])
            kept, kept_value = (returned, estimate_back) if k == local else (hidden, estimate)
            kept[k] = final.astype(jnp.bfloat16)
            value = jnp.tanh(jnp.sum(final * vw_ref[...], axis=-1, keepdims=True))
            kept_value[k] = jnp.transpose(jnp.broadcast_to(value, (BLOCK, BLOCK)))[0:8]
        for k in range(first, first + GROUP):
            if k != local:
                give_back(k)

    for k in range(slots):
        if k != local:
            remote(hidden.at[k], returned.at[k], back_send.at[k], back_recv.at[k], from_peer[k]).wait_recv()
            remote(
                estimate.at[k], estimate_back.at[k], value_send.at[k], value_recv.at[k], from_peer[k]
            ).wait_recv()

    for b in range(bv_ref.shape[0]):
        block, value = returned[0], estimate_back[0]
        for k in range(1, slots):
            chosen = bv_ref[b] == to_peer[k][0]
            block = jnp.where(chosen, returned[k], block)
            value = jnp.where(chosen, estimate_back[k], value)
        hid_out[pl.ds(b * BLOCK, BLOCK), :] = block
        val_out[pl.ds(b, 1), :] = value[0:1]

    for copy in sent:
        copy.wait_send()


def local(
    positions,
    game_counts,
    block_variant,
    norm_gain,
    up_weight,
    down_weight,
    final_gain,
    value_weight,
    policy_weight,
):
    variants, members = lax.axis_size("variant"), lax.axis_size("mp")
    zs = members // (XHI * CORES)
    games_here, width = positions.shape
    blocks = block_variant.shape[0]
    up_rows, ffw = up_weight.shape[1:]
    down_rows = down_weight.shape[1]
    slots = variants
    vmem = pl.BlockSpec(memory_space=pltpu.VMEM)
    dma = pltpu.SemaphoreType.DMA
    policy_whole = lax.all_gather(policy_weight, ("variant", "mp"), axis=0, tiled=True)
    own_hidden, own_value = pl.pallas_call(
        functools.partial(exchange_kernel, variants, members),
        out_shape=(
            jax.ShapeDtypeStruct((games_here, width), jnp.bfloat16),
            jax.ShapeDtypeStruct((blocks, BLOCK), jnp.float32),
        ),
        in_specs=[pl.BlockSpec(memory_space=pltpu.SMEM)] + [vmem] * 6,
        out_specs=(vmem, vmem),
        scratch_shapes=[
            pltpu.VMEM((slots, BLOCK, width), jnp.bfloat16),
            pltpu.VMEM((slots, BLOCK, width), jnp.bfloat16),
            pltpu.VMEM((slots * BLOCK, width), jnp.bfloat16),
            pltpu.VMEM((slots * BLOCK, ffw), jnp.bfloat16),
            pltpu.VMEM((up_rows * members, ffw), jnp.bfloat16),
            pltpu.VMEM((down_rows * members, width), jnp.bfloat16),
            pltpu.VMEM((slots, BLOCK, width), jnp.bfloat16),
            pltpu.VMEM((slots, BLOCK, width), jnp.bfloat16),
            pltpu.VMEM((slots, 8, BLOCK), jnp.float32),
            pltpu.VMEM((slots, 8, BLOCK), jnp.float32),
            dma((2, XHI, zs, CORES)),
            dma((2, XHI, zs)),
            dma((2, XHI, zs)),
            dma((2, XHI, zs)),
            dma((2,)),
            dma((slots,)),
            dma((slots,)),
            dma((slots,)),
            dma((slots,)),
            dma((slots,)),
            dma((slots,)),
        ],
        compiler_params=pltpu.CompilerParams(
            collective_id=0, has_side_effects=True, vmem_limit_bytes=52 * 1024 * 1024
        ),
        cost_estimate=pl.CostEstimate(
            flops=4 * slots * BLOCK * width * ffw, bytes_accessed=4 * width * ffw, transcendentals=0
        ),
        name="exchange",
    )(block_variant, positions, up_weight[0], down_weight[0], norm_gain, final_gain, value_weight)
    logits = jnp.dot(own_hidden, policy_whole, preferred_element_type=jnp.float32).astype(jnp.bfloat16)
    row_live = jnp.arange(games_here, dtype=jnp.int32) < game_counts[0]
    policy = jnp.where(row_live[:, None], logits, jnp.zeros((), jnp.bfloat16))
    value = jnp.where(row_live, own_value.reshape(games_here), jnp.zeros((), jnp.float32))
    return (policy, value)


def solution(mesh):
    in_specs = (
        P(("variant", "mp"), None),
        P(("variant", "mp")),
        P(("variant", "mp")),
        P("variant", None),
        P("variant", "mp", None),
        P("variant", "mp", None),
        P("variant", None),
        P("variant", None),
        P(("variant", "mp"), None),
    )
    out_specs = (P(("variant", "mp"), None), P(("variant", "mp")))
    return jax.shard_map(local, mesh=mesh, in_specs=in_specs, out_specs=out_specs, check_vma=False)
```

```python
import functools

import jax
import jax.numpy as jnp
from jax import lax
from jax.experimental import pallas as pl
from jax.experimental.pallas import tpu as pltpu
from jax.sharding import PartitionSpec as P

MESH = pl.DeviceIdType.MESH
BLOCK = 128
EPS = 1e-06
XLO, XHI, CORES = 2, 2, 2
GROUP = 2


def rms_scale(values, gain):
    mean_square = jnp.mean(values * values, axis=-1, keepdims=True)
    return values * lax.rsqrt(mean_square + EPS) * gain


def remote(src, dst, send_sem, recv_sem, device):
    return pltpu.make_async_remote_copy(
        src_ref=src, dst_ref=dst, send_sem=send_sem, recv_sem=recv_sem, device_id=device, device_id_type=MESH
    )


def exchange_kernel(
    variants,
    members,
    bv_ref,
    pos_ref,
    up_ref,
    down_ref,
    ng_ref,
    fg_ref,
    vw_ref,
    count_ref,
    piece_ref,
    policy_out,
    val_out,
    outgoing,
    incoming,
    normed,
    active,
    up_all,
    down_all,
    hidden,
    returned,
    estimate,
    estimate_back,
    ring_recv,
    plus_send,
    minus_send,
    core_send,
    half_send,
    slot_send,
    slot_recv,
    back_send,
    back_recv,
    value_send,
    value_recv,
    own_hidden,
    policy_all,
    pieces,
    piece_send,
    piece_recv,
    pair_send,
    pair_recv,
    first_send,
    first_recv,
    second_send,
    second_recv,
    policy_core_send,
    policy_core_recv,
):
    ys, zs = variants // XLO, members // (XHI * CORES)
    v, m = lax.axis_index("variant"), lax.axis_index("mp")
    y, xl = lax.div(v, XLO), lax.rem(v, XLO)
    xh, z, core = lax.div(m, zs * CORES), lax.rem(lax.div(m, CORES), zs), lax.rem(m, CORES)

    def member(xr, dz, cr):
        return (lax.rem(xh + xr, XHI) * zs + lax.rem(z + dz, zs)) * CORES + lax.rem(core + cr, CORES)

    def peer(dy, dx):
        return lax.rem(y + dy, ys) * XLO + lax.rem(xl + dx, XLO)

    z_plus, z_minus = (v, member(0, 1, 0)), (v, member(0, zs - 1, 0))
    sibling, half = (v, member(0, 0, 1)), (v, member(1, 0, 0))
    order = sorted(
        ((dy, dx) for dy in range(ys) for dx in range(XLO)), key=lambda r: (-min(r[0], ys - r[0]), -r[1])
    )
    to_peer = [(peer(dy, dx), m) for dy, dx in order]
    from_peer = [(peer(ys - dy, XLO - dx), m) for dy, dx in order]
    slots = len(order)
    local = slots - 1

    half_columns = policy_all.shape[1] // CORES
    tile_rows = piece_ref.shape[0]
    unit_rows = zs // 2 * tile_rows
    paired = z + 1 - 2 * lax.rem(z, 2) - z
    other_z = (v, member(0, zs + paired, 0))
    other_z_sibling = (v, member(0, zs + paired, 1))
    x = xh * XLO + xl
    xs = XHI * XLO

    def chip(cx, cy):
        cx, cy = lax.rem(cx, xs), lax.rem(cy, ys)
        return cy * XLO + lax.rem(cx, XLO), (lax.div(cx, XLO) * zs + z) * CORES + core

    def along(first, second):
        return x + first * (1 - core) + second * core, y + first * core + second * (1 - core)

    first_plus, first_minus = chip(*along(1, 0)), chip(*along(3, 0))
    second_plus, second_minus = chip(*along(0, 1)), chip(*along(0, 3))
    skips = (2, zs - 2, zs // 2)
    skip_to = [(v, member(0, d, 0)) for d in skips]

    def policy_rows(a, b, cr, start=0, count=None):
        axis = lax.rem(core + cr, CORES)
        cx = lax.rem(x + (xs - a) * (1 - axis) + (xs - b) * axis, xs)
        cy = lax.rem(y + (ys - a) * axis + (ys - b) * (1 - axis), ys)
        group = (cy * XLO + lax.rem(cx, XLO)) * XHI + lax.div(cx, XLO)
        row = pl.multiple_of(group * unit_rows + start, tile_rows)
        column = pl.multiple_of(axis * half_columns, 128)
        return policy_all.at[pl.ds(row, unit_rows if count is None else count), pl.ds(column, half_columns)]

    def policy_tile(dz):
        return policy_rows(0, 0, 0, lax.div(lax.rem(z + dz, zs), 2) * tile_rows, tile_rows)

    barrier = pltpu.get_barrier_semaphore()
    greeted = [z_plus, z_minus, sibling, half, *to_peer[:local]]
    greeted += [other_z_sibling, (peer(0, 1), member(1, 0, 0)), *skip_to]
    for device in greeted:
        pl.semaphore_signal(barrier, inc=1, device_id=device, device_id_type=MESH)
    pl.semaphore_wait(barrier, len(greeted))

    shards, wholes = (up_ref, down_ref), (up_all, down_all)

    def rows(kind, xr, dist, cr):
        depth = shards[kind].shape[0]
        owner = member(xr, zs - dist, cr)
        return wholes[kind].at[pl.ds(pl.multiple_of(owner * depth, depth), depth)]

    def source(kind, xr, dist):
        return shards[kind] if (xr, dist) == (0, 0) else rows(kind, xr, dist, 0)

    sent = []

    def send(copy):
        copy.start()
        sent.append(copy)

    def send_half(kind):
        send(remote(shards[kind], rows(kind, 0, 0, 0), half_send.at[kind], ring_recv.at[kind, 1, 0, 0], half))

    def send_plus(kind, xr, dist):
        send(
            remote(
                source(kind, xr, dist),
                rows(kind, xr, dist, 0),
                plus_send.at[kind, xr, dist],
                ring_recv.at[kind, xr, dist + 1, 0],
                z_plus,
            )
        )

    def send_minus(kind, xr, dist):
        send(
            remote(
                source(kind, xr, dist),
                rows(kind, xr, dist, 0),
                minus_send.at[kind, xr, dist],
                ring_recv.at[kind, xr, (dist - 1) % zs, 0],
                z_minus,
            )
        )

    def send_core(kind, xr, dist):
        send(
            remote(
                source(kind, xr, dist),
                rows(kind, xr, dist, 0),
                core_send.at[kind, xr, dist],
                ring_recv.at[kind, xr, dist, 1],
                sibling,
            )
        )

    def arrived(kind, xr, dist, cr):
        ref = rows(kind, xr, dist, cr)
        remote(ref, ref, core_send.at[kind, xr, dist], ring_recv.at[kind, xr, dist, cr], sibling).wait_recv()

    plus = (zs // 2, zs - 1 - zs // 2)
    minus = (zs - 1 - zs // 2, zs // 2)
    steps = zs // 2

    def begin_own(kind):
        send_plus(kind, 0, 0)
        send_minus(kind, 0, 0)
        send_core(kind, 0, 0)

    def begin_half(kind):
        arrived(kind, 1, 0, 0)
        send_plus(kind, 1, 0)
        send_minus(kind, 1, 0)
        send_core(kind, 1, 0)

    def ring_step(kind, step):
        for xr in range(XHI):
            if step <= plus[kind]:
                arrived(kind, xr, step, 0)
                if step < plus[kind]:
                    send_plus(kind, xr, step)
                send_core(kind, xr, step)
            if step <= minus[kind]:
                arrived(kind, xr, zs - step, 0)
                if step < minus[kind]:
                    send_minus(kind, xr, zs - step)
                send_core(kind, xr, zs - step)

    own_columns = pl.ds(pl.multiple_of(core * half_columns, 128), half_columns)
    sibling_columns = pl.ds(pl.multiple_of((1 - core) * half_columns, 128), half_columns)

    def piece_copy(i):
        columns = own_columns if i == 1 else sibling_columns
        device = (sibling, other_z, other_z_sibling)[i]
        return remote(piece_ref.at[:, columns], pieces.at[i], piece_send.at[i], piece_recv.at[i], device)

    def merge_pieces():
        total = piece_ref[:, own_columns].astype(jnp.float32)
        for i in range(3):
            piece_copy(i).wait_recv()
            total = total + pieces[i].astype(jnp.float32)
        policy_tile(0)[...] = total.astype(jnp.bfloat16)

    def skip_copy(i, dz):
        ref = policy_tile(dz)
        return remote(ref, ref, pair_send.at[i], pair_recv.at[i], skip_to[i])

    def send_skips():
        for i in range(len(skips)):
            send(skip_copy(i, 0))

    def policy_to_core(a, b):
        ref = policy_rows(a, b, 0)
        send(remote(ref, ref, policy_core_send.at[a, b], policy_core_recv.at[a, b], sibling))

    part_unit = unit_rows // 2

    def first_copy(i, a):
        ref = policy_rows(a, 0, 0) if i < 2 else policy_rows(a, 0, 0, (i - 2) * part_unit, part_unit)
        return remote(ref, ref, first_send.at[i], first_recv.at[i], (first_plus, first_minus)[i % 2])

    def first_begin():
        for i, dz in enumerate(skips):
            skip_copy(i, zs - dz).wait_recv()
        send(first_copy(0, 0))
        send(first_copy(1, 0))
        policy_to_core(0, 0)

    def first_forward():
        for i, a in ((0, 1), (1, 3)):
            first_copy(i, a).wait_recv()
            send(first_copy(2 + i, a))
            policy_to_core(a, 0)

    def second_copy(a, i, b):
        ref = policy_rows(a, b, 0)
        device = second_plus if i == 0 or (i == 2 and a < 2) else second_minus
        return remote(ref, ref, second_send.at[a, i], second_recv.at[a, i], device)

    def second_begin():
        for i in (2, 3):
            first_copy(i, 2).wait_recv()
        policy_to_core(2, 0)
        for a in range(xs):
            send(second_copy(a, 0, 0))
            send(second_copy(a, 1, 0))

    def second_forward():
        for a in range(xs):
            for i, b in ((0, 1), (1, 3)):
                second_copy(a, i, b).wait_recv()
                if (i == 0) == (a < 2):
                    send(second_copy(a, 2, b))
                policy_to_core(a, b)

    def second_end():
        for a in range(xs):
            second_copy(a, 2, 2).wait_recv()
            policy_to_core(a, 2)

    for i in range(3):
        send(piece_copy(i))
    send_half(0)
    begin_own(0)
    send_half(1)

    def fill(k):
        wanted = to_peer[k][0]
        block = pos_ref[0:BLOCK, :]
        for b in range(1, bv_ref.shape[0]):
            block = jnp.where(bv_ref[b] == wanted, pos_ref[b * BLOCK : (b + 1) * BLOCK, :], block)
        if k == local:
            incoming[k] = block
        else:
            outgoing[k] = block

    def dispatch(k):
        send(remote(outgoing.at[k], incoming.at[k], slot_send.at[k], slot_recv.at[k], to_peer[k]))

    for k in range(slots):
        fill(k)
    dispatch(0)
    dispatch(1)

    for kind in range(2):
        depth = shards[kind].shape[0]
        wholes[kind][pl.ds(pl.multiple_of(m * depth, depth), depth), :] = shards[kind][...]

    merge_pieces()
    begin_half(0)
    ring_step(0, 1)
    send_skips()
    ring_step(0, 2)
    first_begin()
    for k in range(2, local):
        dispatch(k)
    for step in range(3, steps):
        ring_step(0, step)
    begin_own(1)
    begin_half(1)
    ring_step(0, steps)
    first_forward()
    ring_step(1, 1)
    second_begin()
    for step in range(2, steps):
        ring_step(1, step)

    for k in range(slots):
        if k != local:
            remote(outgoing.at[k], incoming.at[k], slot_send.at[k], slot_recv.at[k], to_peer[k]).wait_recv()
        normed[pl.ds(k * BLOCK, BLOCK), :] = rms_scale(incoming[k].astype(jnp.float32), ng_ref[...]).astype(
            jnp.bfloat16
        )
    for xr in range(XHI):
        for dist in range(zs):
            arrived(0, xr, dist, 1)

    total_rows = normed.shape[0]
    part_rows = total_rows // 2
    width = 256
    tiles = up_all.shape[1] // width

    def up_tiles(first, last):
        def one(i, carry):
            col = pl.multiple_of(lax.div(i, 2) * width, width)
            row = pl.multiple_of(lax.rem(i, 2) * part_rows, part_rows)
            upward = jnp.dot(
                normed[pl.ds(row, part_rows), :],
                up_all[:, pl.ds(col, width)],
                preferred_element_type=jnp.float32,
            )
            active[pl.ds(row, part_rows), pl.ds(col, width)] = jax.nn.gelu(upward, approximate=True).astype(
                jnp.bfloat16
            )
            return carry

        lax.fori_loop(2 * first, 2 * last, one, 0)

    up_tiles(0, tiles // 2)
    ring_step(1, steps)
    second_forward()
    up_tiles(tiles // 2, tiles)
    for xr in range(XHI):
        for dist in range(zs):
            arrived(1, xr, dist, 1)

    def give_back(k):
        send(remote(hidden.at[k], returned.at[k], back_send.at[k], back_recv.at[k], from_peer[k]))
        send(remote(estimate.at[k], estimate_back.at[k], value_send.at[k], value_recv.at[k], from_peer[k]))

    for first in range(0, slots, GROUP):
        downward = jnp.dot(
            active[pl.ds(first * BLOCK, GROUP * BLOCK), :], down_all[...], preferred_element_type=jnp.float32
        )
        for k in range(first, first + GROUP):
            part = downward[(k - first) * BLOCK : (k - first + 1) * BLOCK]
            final = rms_scale(incoming[k].astype(jnp.float32) + part, fg_ref[...])
            kept, kept_value = (returned, estimate_back) if k == local else (hidden, estimate)
            kept[k] = final.astype(jnp.bfloat16)
            value = jnp.tanh(jnp.sum(final * vw_ref[...], axis=-1, keepdims=True))
            kept_value[k] = jnp.transpose(jnp.broadcast_to(value, (BLOCK, BLOCK)))[0:8]
        for k in range(first, first + GROUP):
            if k != local:
                give_back(k)

    second_end()
    for k in range(slots):
        if k != local:
            remote(hidden.at[k], returned.at[k], back_send.at[k], back_recv.at[k], from_peer[k]).wait_recv()
            remote(
                estimate.at[k], estimate_back.at[k], value_send.at[k], value_recv.at[k], from_peer[k]
            ).wait_recv()
    for a in range(xs):
        for b in range(ys):
            ref = policy_rows(a, b, 1)
            remote(ref, ref, policy_core_send.at[a, b], policy_core_recv.at[a, b], sibling).wait_recv()

    count = count_ref[0]
    for b in range(bv_ref.shape[0]):
        block, value = returned[0], estimate_back[0]
        for k in range(1, slots):
            chosen = bv_ref[b] == to_peer[k][0]
            block = jnp.where(chosen, returned[k], block)
            value = jnp.where(chosen, estimate_back[k], value)
        own_hidden[pl.ds(b * BLOCK, BLOCK), :] = block
        games = b * BLOCK + lax.broadcasted_iota(jnp.int32, (1, BLOCK), 1)
        val_out[pl.ds(b, 1), :] = jnp.where(games < count, value[0:1], 0.0)

    games_here, moves = policy_out.shape
    live = lax.broadcasted_iota(jnp.int32, (games_here, 1), 0) < count

    def masked_logits(columns):
        logits = jnp.dot(own_hidden[...], policy_all[:, columns], preferred_element_type=jnp.float32)
        return jnp.where(live, logits, 0.0).astype(jnp.bfloat16)

    whole_tiles = moves // width

    def policy_tile_step(i, carry):
        columns = pl.ds(pl.multiple_of(i * width, width), width)
        policy_out[:, columns] = masked_logits(columns)
        return carry

    lax.fori_loop(0, whole_tiles, policy_tile_step, 0)
    rest = moves - whole_tiles * width
    if rest:
        policy_out[:, pl.ds(whole_tiles * width, rest)] = masked_logits(pl.ds(whole_tiles * width, width))[:, :rest]

    for copy in sent:
        copy.wait_send()


def local(
    positions,
    game_counts,
    block_variant,
    norm_gain,
    up_weight,
    down_weight,
    final_gain,
    value_weight,
    policy_weight,
):
    variants, members = lax.axis_size("variant"), lax.axis_size("mp")
    zs = members // (XHI * CORES)
    games_here, width = positions.shape
    blocks = block_variant.shape[0]
    up_rows, ffw = up_weight.shape[1:]
    down_rows = down_weight.shape[1]
    slots = variants
    vmem = pl.BlockSpec(memory_space=pltpu.VMEM)
    dma = pltpu.SemaphoreType.DMA
    policy_rows_here, moves = policy_weight.shape
    half_columns = -(-moves // (CORES * 128)) * 128
    tile_rows = 2 * CORES * policy_rows_here
    widened = jnp.pad(policy_weight, ((0, 0), (0, CORES * half_columns - moves)))
    place = lax.rem(lax.axis_index("mp"), 2 * CORES)
    in_place = lax.div(jnp.arange(tile_rows, dtype=jnp.int32), policy_rows_here) == place
    piece = jnp.where(in_place[:, None], jnp.tile(widened, (2 * CORES, 1)), jnp.zeros((), jnp.bfloat16))
    policy, value = pl.pallas_call(
        functools.partial(exchange_kernel, variants, members),
        out_shape=(
            jax.ShapeDtypeStruct((games_here, moves), jnp.bfloat16),
            jax.ShapeDtypeStruct((blocks, BLOCK), jnp.float32),
        ),
        in_specs=[pl.BlockSpec(memory_space=pltpu.SMEM)]
        + [vmem] * 6
        + [pl.BlockSpec(memory_space=pltpu.SMEM), vmem],
        out_specs=(vmem, vmem),
        scratch_shapes=[
            pltpu.VMEM((slots, BLOCK, width), jnp.bfloat16),
            pltpu.VMEM((slots, BLOCK, width), jnp.bfloat16),
            pltpu.VMEM((slots * BLOCK, width), jnp.bfloat16),
            pltpu.VMEM((slots * BLOCK, ffw), jnp.bfloat16),
            pltpu.VMEM((up_rows * members, ffw), jnp.bfloat16),
            pltpu.VMEM((down_rows * members, width), jnp.bfloat16),
            pltpu.VMEM((slots, BLOCK, width), jnp.bfloat16),
            pltpu.VMEM((slots, BLOCK, width), jnp.bfloat16),
            pltpu.VMEM((slots, 8, BLOCK), jnp.float32),
            pltpu.VMEM((slots, 8, BLOCK), jnp.float32),
            dma((2, XHI, zs, CORES)),
            dma((2, XHI, zs)),
            dma((2, XHI, zs)),
            dma((2, XHI, zs)),
            dma((2,)),
            dma((slots,)),
            dma((slots,)),
            dma((slots,)),
            dma((slots,)),
            dma((slots,)),
            dma((slots,)),
            pltpu.VMEM((games_here, width), jnp.bfloat16),
            pltpu.VMEM((variants * members * policy_rows_here, CORES * half_columns), jnp.bfloat16),
            pltpu.VMEM((3, tile_rows, half_columns), jnp.bfloat16),
            dma((3,)),
            dma((3,)),
            dma((3,)),
            dma((3,)),
            dma((4,)),
            dma((4,)),
            dma((4, 3)),
            dma((4, 3)),
            dma((4, 4)),
            dma((4, 4)),
        ],
        compiler_params=pltpu.CompilerParams(
            collective_id=0, has_side_effects=True, vmem_limit_bytes=58 * 1024 * 1024
        ),
        cost_estimate=pl.CostEstimate(
            flops=4 * slots * BLOCK * width * ffw, bytes_accessed=4 * width * ffw, transcendentals=0
        ),
        name="exchange",
    )(
        block_variant,
        positions,
        up_weight[0],
        down_weight[0],
        norm_gain,
        final_gain,
        value_weight,
        game_counts,
        piece,
    )
    return (policy, value.reshape(games_here))


def solution(mesh):
    in_specs = (
        P(("variant", "mp"), None),
        P(("variant", "mp")),
        P(("variant", "mp")),
        P("variant", None),
        P("variant", "mp", None),
        P("variant", "mp", None),
        P("variant", None),
        P("variant", None),
        P(("variant", "mp"), None),
    )
    out_specs = (P(("variant", "mp"), None), P(("variant", "mp")))
    return jax.shard_map(local, mesh=mesh, in_specs=in_specs, out_specs=out_specs, check_vma=False)
```

```python
import functools

import jax
import jax.numpy as jnp
from jax import lax
from jax.experimental import pallas as pl
from jax.experimental.pallas import tpu as pltpu
from jax.sharding import PartitionSpec as P

MESH = pl.DeviceIdType.MESH
BLOCK = 128
EPS = 1e-06
XLO, XHI, CORES = 2, 2, 2
GROUP = 2


def rms_scale(values, gain):
    mean_square = jnp.mean(values * values, axis=-1, keepdims=True)
    return values * lax.rsqrt(mean_square + EPS) * gain


def remote(src, dst, send_sem, recv_sem, device):
    return pltpu.make_async_remote_copy(
        src_ref=src, dst_ref=dst, send_sem=send_sem, recv_sem=recv_sem, device_id=device, device_id_type=MESH
    )


def exchange_kernel(
    variants,
    members,
    bv_ref,
    pos_ref,
    up_ref,
    down_ref,
    ng_ref,
    fg_ref,
    vw_ref,
    count_ref,
    piece_ref,
    policy_out,
    val_out,
    outgoing,
    incoming,
    normed,
    active,
    up_all,
    down_all,
    hidden,
    returned,
    estimate,
    estimate_back,
    ring_recv,
    plus_send,
    minus_send,
    core_send,
    half_send,
    slot_send,
    slot_recv,
    back_send,
    back_recv,
    value_send,
    value_recv,
    own_hidden,
    policy_all,
    pieces,
    piece_send,
    piece_recv,
    pair_send,
    pair_recv,
    first_send,
    first_recv,
    second_send,
    second_recv,
    policy_core_send,
    policy_core_recv,
):
    ys, zs = variants // XLO, members // (XHI * CORES)
    v, m = lax.axis_index("variant"), lax.axis_index("mp")
    y, xl = lax.div(v, XLO), lax.rem(v, XLO)
    xh, z, core = lax.div(m, zs * CORES), lax.rem(lax.div(m, CORES), zs), lax.rem(m, CORES)

    def member(xr, dz, cr):
        return (lax.rem(xh + xr, XHI) * zs + lax.rem(z + dz, zs)) * CORES + lax.rem(core + cr, CORES)

    def peer(dy, dx):
        return lax.rem(y + dy, ys) * XLO + lax.rem(xl + dx, XLO)

    z_plus, z_minus = (v, member(0, 1, 0)), (v, member(0, zs - 1, 0))
    sibling, half = (v, member(0, 0, 1)), (v, member(1, 0, 0))
    order = sorted(
        ((dy, dx) for dy in range(ys) for dx in range(XLO)), key=lambda r: (-min(r[0], ys - r[0]), -r[1])
    )
    to_peer = [(peer(dy, dx), m) for dy, dx in order]
    from_peer = [(peer(ys - dy, XLO - dx), m) for dy, dx in order]
    slots = len(order)
    local = slots - 1

    half_columns = policy_all.shape[1] // CORES
    tile_rows = piece_ref.shape[0]
    unit_rows = zs // 2 * tile_rows
    paired = z + 1 - 2 * lax.rem(z, 2) - z
    other_z = (v, member(0, zs + paired, 0))
    other_z_sibling = (v, member(0, zs + paired, 1))
    x = xh * XLO + xl
    xs = XHI * XLO

    def chip(cx, cy):
        cx, cy = lax.rem(cx, xs), lax.rem(cy, ys)
        return cy * XLO + lax.rem(cx, XLO), (lax.div(cx, XLO) * zs + z) * CORES + core

    def along(first, second):
        return x + first * (1 - core) + second * core, y + first * core + second * (1 - core)

    first_plus, first_minus = chip(*along(1, 0)), chip(*along(3, 0))
    second_plus, second_minus = chip(*along(0, 1)), chip(*along(0, 3))
    skips = (2, zs - 2, zs // 2)
    skip_to = [(v, member(0, d, 0)) for d in skips]

    def policy_rows(a, b, cr, start=0, count=None):
        axis = lax.rem(core + cr, CORES)
        cx = lax.rem(x + (xs - a) * (1 - axis) + (xs - b) * axis, xs)
        cy = lax.rem(y + (ys - a) * axis + (ys - b) * (1 - axis), ys)
        group = (cy * XLO + lax.rem(cx, XLO)) * XHI + lax.div(cx, XLO)
        row = pl.multiple_of(group * unit_rows + start, tile_rows)
        column = pl.multiple_of(axis * half_columns, 128)
        return policy_all.at[pl.ds(row, unit_rows if count is None else count), pl.ds(column, half_columns)]

    def policy_tile(dz):
        return policy_rows(0, 0, 0, lax.div(lax.rem(z + dz, zs), 2) * tile_rows, tile_rows)

    barrier = pltpu.get_barrier_semaphore()
    greeted = [z_plus, z_minus, sibling, half, *to_peer[:local]]
    greeted += [other_z_sibling, (peer(0, 1), member(1, 0, 0)), *skip_to]
    for device in greeted:
        pl.semaphore_signal(barrier, inc=1, device_id=device, device_id_type=MESH)
    pl.semaphore_wait(barrier, len(greeted))

    shards, wholes = (up_ref, down_ref), (up_all, down_all)

    up_pieces, down_pieces = (0, 1), (2, 3)

    def rows(piece, xr, dist, cr):
        kind, part = divmod(piece, 2)
        depth = shards[kind].shape[0]
        owner = member(xr, zs - dist, cr)
        start = pl.multiple_of(owner * depth + part * (depth // 2), depth // 2)
        return wholes[kind].at[pl.ds(start, depth // 2)]

    def own(piece):
        kind, part = divmod(piece, 2)
        depth = shards[kind].shape[0]
        return shards[kind].at[pl.ds(part * (depth // 2), depth // 2)]

    def source(piece, xr, dist):
        return own(piece) if (xr, dist) == (0, 0) else rows(piece, xr, dist, 0)

    sent = []

    def send(copy):
        copy.start()
        sent.append(copy)

    def send_half(piece):
        send(remote(own(piece), rows(piece, 0, 0, 0), half_send.at[piece], ring_recv.at[piece, 1, 0, 0], half))

    def ring_send(piece, xr, dist, sems, dist_there, cr_there, device):
        send(
            remote(
                source(piece, xr, dist),
                rows(piece, xr, dist, 0),
                sems.at[piece, xr, dist],
                ring_recv.at[piece, xr, dist_there, cr_there],
                device,
            )
        )

    def send_plus(piece, xr, dist):
        ring_send(piece, xr, dist, plus_send, dist + 1, 0, z_plus)

    def send_minus(piece, xr, dist):
        ring_send(piece, xr, dist, minus_send, (dist - 1) % zs, 0, z_minus)

    def send_core(piece, xr, dist):
        ring_send(piece, xr, dist, core_send, dist, 1, sibling)

    def arrived(piece, xr, dist, cr):
        ref = rows(piece, xr, dist, cr)
        remote(ref, ref, core_send.at[piece, xr, dist], ring_recv.at[piece, xr, dist, cr], sibling).wait_recv()

    plus = (zs // 2, zs - 1 - zs // 2)
    minus = (zs - 1 - zs // 2, zs // 2)
    steps = zs // 2

    def begin(pieces_here, xr):
        for piece in pieces_here:
            if xr:
                arrived(piece, xr, 0, 0)
            send_plus(piece, xr, 0)
            send_minus(piece, xr, 0)
        for piece in pieces_here:
            send_core(piece, xr, 0)

    def ring_step(pieces_here, step, halves=(0, 1), between=None):
        kind = pieces_here[0] // 2
        for xr in halves:
            for piece in pieces_here:
                if step <= plus[kind]:
                    arrived(piece, xr, step, 0)
                    if step < plus[kind]:
                        send_plus(piece, xr, step)
                    send_core(piece, xr, step)
                if step <= minus[kind]:
                    arrived(piece, xr, zs - step, 0)
                    if step < minus[kind]:
                        send_minus(piece, xr, zs - step)
                    send_core(piece, xr, zs - step)
                if between is not None:
                    between()

    own_columns = pl.ds(pl.multiple_of(core * half_columns, 128), half_columns)
    sibling_columns = pl.ds(pl.multiple_of((1 - core) * half_columns, 128), half_columns)

    def piece_copy(i):
        columns = own_columns if i == 1 else sibling_columns
        device = (sibling, other_z, other_z_sibling)[i]
        return remote(piece_ref.at[:, columns], pieces.at[i], piece_send.at[i], piece_recv.at[i], device)

    def merge_pieces():
        total = piece_ref[:, own_columns].astype(jnp.float32)
        for i in range(3):
            piece_copy(i).wait_recv()
            total = total + pieces[i].astype(jnp.float32)
        policy_tile(0)[...] = total.astype(jnp.bfloat16)

    def skip_copy(i, dz):
        ref = policy_tile(dz)
        return remote(ref, ref, pair_send.at[i], pair_recv.at[i], skip_to[i])

    def send_skips():
        for i in range(len(skips)):
            send(skip_copy(i, 0))

    def policy_to_core(a, b):
        ref = policy_rows(a, b, 0)
        send(remote(ref, ref, policy_core_send.at[a, b], policy_core_recv.at[a, b], sibling))

    part_unit = unit_rows // 2

    def first_copy(i, a):
        ref = policy_rows(a, 0, 0) if i < 2 else policy_rows(a, 0, 0, (i - 2) * part_unit, part_unit)
        return remote(ref, ref, first_send.at[i], first_recv.at[i], (first_plus, first_minus)[i % 2])

    def first_begin():
        for i, dz in enumerate(skips):
            skip_copy(i, zs - dz).wait_recv()
        send(first_copy(0, 0))
        send(first_copy(1, 0))
        policy_to_core(0, 0)

    def first_forward():
        for i, a in ((0, 1), (1, 3)):
            first_copy(i, a).wait_recv()
            send(first_copy(2 + i, a))
            policy_to_core(a, 0)

    def second_copy(a, i, b):
        ref = policy_rows(a, b, 0)
        device = second_plus if i == 0 or (i == 2 and a < 2) else second_minus
        return remote(ref, ref, second_send.at[a, i], second_recv.at[a, i], device)

    def second_begin():
        for i in (2, 3):
            first_copy(i, 2).wait_recv()
        policy_to_core(2, 0)
        for a in range(xs):
            send(second_copy(a, 0, 0))
            send(second_copy(a, 1, 0))

    def second_forward():
        for a in range(xs):
            for i, b in ((0, 1), (1, 3)):
                second_copy(a, i, b).wait_recv()
                if (i == 0) == (a < 2):
                    send(second_copy(a, 2, b))
                policy_to_core(a, b)

    def second_end():
        for a in range(xs):
            second_copy(a, 2, 2).wait_recv()
            policy_to_core(a, 2)

    for i in range(3):
        send(piece_copy(i))
    for piece in up_pieces:
        send_half(piece)
    begin(up_pieces, 0)
    for piece in down_pieces:
        send_half(piece)
    begin(down_pieces, 0)

    def fill(k):
        wanted = to_peer[k][0]
        block = pos_ref[0:BLOCK, :]
        for b in range(1, bv_ref.shape[0]):
            block = jnp.where(bv_ref[b] == wanted, pos_ref[b * BLOCK : (b + 1) * BLOCK, :], block)
        if k == local:
            incoming[k] = block
        else:
            outgoing[k] = block

    def dispatch(k):
        send(remote(outgoing.at[k], incoming.at[k], slot_send.at[k], slot_recv.at[k], to_peer[k]))

    for k in range(slots):
        fill(k)
    early = slots // 2
    for k in range(early):
        dispatch(k)

    for kind in range(2):
        depth = shards[kind].shape[0]
        wholes[kind][pl.ds(pl.multiple_of(m * depth, depth), depth), :] = shards[kind][...]

    total_rows = normed.shape[0]
    part_rows = total_rows // 2
    width = 256
    up_parts = 2 * (up_all.shape[1] // width)
    made = []

    def up_part():
        index = len(made)
        if index >= up_parts:
            return
        made.append(index)
        column_rows = pl.ds(index % 2 * part_rows, part_rows)
        columns = pl.ds(index // 2 * width, width)
        upward = jnp.dot(normed[column_rows, :], up_all[:, columns], preferred_element_type=jnp.float32)
        active[column_rows, columns] = jax.nn.gelu(upward, approximate=True).astype(jnp.bfloat16)

    merge_pieces()
    begin(up_pieces, 1)
    ring_step(up_pieces, 1)
    send_skips()
    begin(down_pieces, 1)
    ring_step(up_pieces, 2)
    first_begin()
    for k in range(early, local):
        dispatch(k)
    ring_step(down_pieces, 1, (0,))
    for step in range(3, steps):
        ring_step(up_pieces, step)
    ring_step(down_pieces, 1, (1,))
    ring_step(up_pieces, steps)
    first_forward()
    ring_step(down_pieces, 2)
    second_begin()

    for k in range(slots):
        if k != local:
            remote(outgoing.at[k], incoming.at[k], slot_send.at[k], slot_recv.at[k], to_peer[k]).wait_recv()
        normed[pl.ds(k * BLOCK, BLOCK), :] = rms_scale(incoming[k].astype(jnp.float32), ng_ref[...]).astype(
            jnp.bfloat16
        )
    for piece in up_pieces:
        for xr in range(XHI):
            for dist in range(zs):
                arrived(piece, xr, dist, 1)

    for step in range(3, steps):
        ring_step(down_pieces, step, between=up_part)
    for _ in range(up_parts // 4):
        up_part()
    ring_step(down_pieces, steps, between=up_part)
    second_forward()
    for _ in range(up_parts):
        up_part()
    for piece in down_pieces:
        for xr in range(XHI):
            for dist in range(zs):
                arrived(piece, xr, dist, 1)

    def give_back(k):
        send(remote(hidden.at[k], returned.at[k], back_send.at[k], back_recv.at[k], from_peer[k]))
        send(remote(estimate.at[k], estimate_back.at[k], value_send.at[k], value_recv.at[k], from_peer[k]))

    for first in range(0, slots, GROUP):
        downward = jnp.dot(
            active[pl.ds(first * BLOCK, GROUP * BLOCK), :], down_all[...], preferred_element_type=jnp.float32
        )
        for k in range(first, first + GROUP):
            part = downward[(k - first) * BLOCK : (k - first + 1) * BLOCK]
            final = rms_scale(incoming[k].astype(jnp.float32) + part, fg_ref[...])
            kept, kept_value = (returned, estimate_back) if k == local else (hidden, estimate)
            kept[k] = final.astype(jnp.bfloat16)
            value = jnp.tanh(jnp.sum(final * vw_ref[...], axis=-1, keepdims=True))
            kept_value[k] = jnp.transpose(jnp.broadcast_to(value, (BLOCK, BLOCK)))[0:8]
        for k in range(first, first + GROUP):
            if k != local:
                give_back(k)

    second_end()
    for k in range(slots):
        if k != local:
            remote(hidden.at[k], returned.at[k], back_send.at[k], back_recv.at[k], from_peer[k]).wait_recv()
            remote(
                estimate.at[k], estimate_back.at[k], value_send.at[k], value_recv.at[k], from_peer[k]
            ).wait_recv()
    for a in range(xs):
        for b in range(ys):
            ref = policy_rows(a, b, 1)
            remote(ref, ref, policy_core_send.at[a, b], policy_core_recv.at[a, b], sibling).wait_recv()

    count = count_ref[0]
    for b in range(bv_ref.shape[0]):
        block, value = returned[0], estimate_back[0]
        for k in range(1, slots):
            chosen = bv_ref[b] == to_peer[k][0]
            block = jnp.where(chosen, returned[k], block)
            value = jnp.where(chosen, estimate_back[k], value)
        own_hidden[pl.ds(b * BLOCK, BLOCK), :] = block
        games = b * BLOCK + lax.broadcasted_iota(jnp.int32, (1, BLOCK), 1)
        val_out[pl.ds(b, 1), :] = jnp.where(games < count, value[0:1], 0.0)

    games_here, moves = policy_out.shape
    live = lax.broadcasted_iota(jnp.int32, (games_here, 1), 0) < count

    def masked_logits(columns):
        logits = jnp.dot(own_hidden[...], policy_all[:, columns], preferred_element_type=jnp.float32)
        return jnp.where(live, logits, 0.0).astype(jnp.bfloat16)

    whole_tiles = moves // width

    def policy_tile_step(i, carry):
        columns = pl.ds(pl.multiple_of(i * width, width), width)
        policy_out[:, columns] = masked_logits(columns)
        return carry

    lax.fori_loop(0, whole_tiles, policy_tile_step, 0)
    rest = moves - whole_tiles * width
    if rest:
        policy_out[:, pl.ds(whole_tiles * width, rest)] = masked_logits(pl.ds(whole_tiles * width, width))[:, :rest]

    for copy in sent:
        copy.wait_send()


def local(
    positions,
    game_counts,
    block_variant,
    norm_gain,
    up_weight,
    down_weight,
    final_gain,
    value_weight,
    policy_weight,
):
    variants, members = lax.axis_size("variant"), lax.axis_size("mp")
    zs = members // (XHI * CORES)
    games_here, width = positions.shape
    blocks = block_variant.shape[0]
    up_rows, ffw = up_weight.shape[1:]
    down_rows = down_weight.shape[1]
    slots = variants
    vmem = pl.BlockSpec(memory_space=pltpu.VMEM)
    dma = pltpu.SemaphoreType.DMA
    policy_rows_here, moves = policy_weight.shape
    half_columns = -(-moves // (CORES * 128)) * 128
    tile_rows = 2 * CORES * policy_rows_here
    widened = jnp.pad(policy_weight, ((0, 0), (0, CORES * half_columns - moves)))
    place = lax.rem(lax.axis_index("mp"), 2 * CORES)
    in_place = lax.div(jnp.arange(tile_rows, dtype=jnp.int32), policy_rows_here) == place
    piece = jnp.where(in_place[:, None], jnp.tile(widened, (2 * CORES, 1)), jnp.zeros((), jnp.bfloat16))
    policy, value = pl.pallas_call(
        functools.partial(exchange_kernel, variants, members),
        out_shape=(
            jax.ShapeDtypeStruct((games_here, moves), jnp.bfloat16),
            jax.ShapeDtypeStruct((blocks, BLOCK), jnp.float32),
        ),
        in_specs=[pl.BlockSpec(memory_space=pltpu.SMEM)]
        + [vmem] * 6
        + [pl.BlockSpec(memory_space=pltpu.SMEM), vmem],
        out_specs=(vmem, vmem),
        scratch_shapes=[
            pltpu.VMEM((slots, BLOCK, width), jnp.bfloat16),
            pltpu.VMEM((slots, BLOCK, width), jnp.bfloat16),
            pltpu.VMEM((slots * BLOCK, width), jnp.bfloat16),
            pltpu.VMEM((slots * BLOCK, ffw), jnp.bfloat16),
            pltpu.VMEM((up_rows * members, ffw), jnp.bfloat16),
            pltpu.VMEM((down_rows * members, width), jnp.bfloat16),
            pltpu.VMEM((slots, BLOCK, width), jnp.bfloat16),
            pltpu.VMEM((slots, BLOCK, width), jnp.bfloat16),
            pltpu.VMEM((slots, 8, BLOCK), jnp.float32),
            pltpu.VMEM((slots, 8, BLOCK), jnp.float32),
            dma((4, XHI, zs, CORES)),
            dma((4, XHI, zs)),
            dma((4, XHI, zs)),
            dma((4, XHI, zs)),
            dma((4,)),
            dma((slots,)),
            dma((slots,)),
            dma((slots,)),
            dma((slots,)),
            dma((slots,)),
            dma((slots,)),
            pltpu.VMEM((games_here, width), jnp.bfloat16),
            pltpu.VMEM((variants * members * policy_rows_here, CORES * half_columns), jnp.bfloat16),
            pltpu.VMEM((3, tile_rows, half_columns), jnp.bfloat16),
            dma((3,)),
            dma((3,)),
            dma((3,)),
            dma((3,)),
            dma((4,)),
            dma((4,)),
            dma((4, 3)),
            dma((4, 3)),
            dma((4, 4)),
            dma((4, 4)),
        ],
        compiler_params=pltpu.CompilerParams(
            collective_id=0, has_side_effects=True, vmem_limit_bytes=58 * 1024 * 1024
        ),
        cost_estimate=pl.CostEstimate(
            flops=4 * slots * BLOCK * width * ffw, bytes_accessed=4 * width * ffw, transcendentals=0
        ),
        name="exchange",
    )(
        block_variant,
        positions,
        up_weight[0],
        down_weight[0],
        norm_gain,
        final_gain,
        value_weight,
        game_counts,
        piece,
    )
    return (policy, value.reshape(games_here))


def solution(mesh):
    in_specs = (
        P(("variant", "mp"), None),
        P(("variant", "mp")),
        P(("variant", "mp")),
        P("variant", None),
        P("variant", "mp", None),
        P("variant", "mp", None),
        P("variant", None),
        P("variant", None),
        P(("variant", "mp"), None),
    )
    out_specs = (P(("variant", "mp"), None), P(("variant", "mp")))
    return jax.shard_map(local, mesh=mesh, in_specs=in_specs, out_specs=out_specs, check_vma=False)
```

```python
import functools

import jax
import jax.numpy as jnp
from jax import lax
from jax.experimental import pallas as pl
from jax.experimental.pallas import tpu as pltpu
from jax.sharding import PartitionSpec as P

MESH = pl.DeviceIdType.MESH
BLOCK = 128
EPS = 1e-06
XLO, XHI, CORES = 2, 2, 2
GROUP = 2


def rms_scale(values, gain):
    mean_square = jnp.mean(values * values, axis=-1, keepdims=True)
    return values * lax.rsqrt(mean_square + EPS) * gain


def remote(src, dst, send_sem, recv_sem, device):
    return pltpu.make_async_remote_copy(
        src_ref=src, dst_ref=dst, send_sem=send_sem, recv_sem=recv_sem, device_id=device, device_id_type=MESH
    )


def exchange_kernel(
    variants,
    members,
    bv_ref,
    pos_ref,
    up_ref,
    down_ref,
    ng_ref,
    fg_ref,
    vw_ref,
    count_ref,
    rows_ref,
    policy_out,
    val_out,
    outgoing,
    incoming,
    normed,
    active,
    up_all,
    down_all,
    hidden,
    returned,
    estimate,
    estimate_back,
    ring_recv,
    plus_send,
    minus_send,
    core_send,
    half_send,
    slot_send,
    slot_recv,
    back_send,
    back_recv,
    value_send,
    value_recv,
    piece_ref,
    policy_all,
    pieces,
    piece_send,
    piece_recv,
    pair_send,
    pair_recv,
    first_send,
    first_recv,
    second_send,
    second_recv,
    policy_core_send,
    policy_core_recv,
):
    ys, zs = variants // XLO, members // (XHI * CORES)
    v, m = lax.axis_index("variant"), lax.axis_index("mp")
    y, xl = lax.div(v, XLO), lax.rem(v, XLO)
    xh, z, core = lax.div(m, zs * CORES), lax.rem(lax.div(m, CORES), zs), lax.rem(m, CORES)

    def member(xr, dz, cr):
        return (lax.rem(xh + xr, XHI) * zs + lax.rem(z + dz, zs)) * CORES + lax.rem(core + cr, CORES)

    def peer(dy, dx):
        return lax.rem(y + dy, ys) * XLO + lax.rem(xl + dx, XLO)

    z_plus, z_minus = (v, member(0, 1, 0)), (v, member(0, zs - 1, 0))
    sibling, half = (v, member(0, 0, 1)), (v, member(1, 0, 0))
    order = sorted(
        ((dy, dx) for dy in range(ys) for dx in range(XLO)), key=lambda r: (-min(r[0], ys - r[0]), -r[1])
    )
    to_peer = [(peer(dy, dx), m) for dy, dx in order]
    from_peer = [(peer(ys - dy, XLO - dx), m) for dy, dx in order]
    slots = len(order)
    local = slots - 1

    half_columns = policy_all.shape[1] // CORES
    tile_rows = piece_ref.shape[0]
    unit_rows = zs // 2 * tile_rows
    paired = z + 1 - 2 * lax.rem(z, 2) - z
    other_z = (v, member(0, zs + paired, 0))
    other_z_sibling = (v, member(0, zs + paired, 1))
    x = xh * XLO + xl
    xs = XHI * XLO

    def chip(cx, cy):
        cx, cy = lax.rem(cx, xs), lax.rem(cy, ys)
        return cy * XLO + lax.rem(cx, XLO), (lax.div(cx, XLO) * zs + z) * CORES + core

    def along(first, second):
        return x + first * (1 - core) + second * core, y + first * core + second * (1 - core)

    first_plus, first_minus = chip(*along(1, 0)), chip(*along(3, 0))
    second_plus, second_minus = chip(*along(0, 1)), chip(*along(0, 3))
    skips = (2, zs - 2, zs // 2)
    skip_to = [(v, member(0, d, 0)) for d in skips]

    def policy_rows(a, b, cr, start=0, count=None):
        axis = lax.rem(core + cr, CORES)
        cx = lax.rem(x + (xs - a) * (1 - axis) + (xs - b) * axis, xs)
        cy = lax.rem(y + (ys - a) * axis + (ys - b) * (1 - axis), ys)
        group = (cy * XLO + lax.rem(cx, XLO)) * XHI + lax.div(cx, XLO)
        row = pl.multiple_of(group * unit_rows + start, tile_rows)
        column = pl.multiple_of(axis * half_columns, 128)
        return policy_all.at[pl.ds(row, unit_rows if count is None else count), pl.ds(column, half_columns)]

    def policy_tile(dz):
        return policy_rows(0, 0, 0, lax.div(lax.rem(z + dz, zs), 2) * tile_rows, tile_rows)

    barrier = pltpu.get_barrier_semaphore()
    greeted = [z_plus, z_minus, sibling, half, *to_peer[:local], other_z_sibling, (peer(0, 1), member(1, 0, 0)), *skip_to]
    for device in greeted:
        pl.semaphore_signal(barrier, inc=1, device_id=device, device_id_type=MESH)

    shards, wholes = (up_ref, down_ref), (up_all, down_all)

    up_pieces, down_pieces = (0, 1), (2, 3)

    def rows(piece, xr, dist, cr):
        kind, part = divmod(piece, 2)
        depth = shards[kind].shape[0]
        owner = member(xr, zs - dist, cr)
        start = pl.multiple_of(owner * depth + part * (depth // 2), depth // 2)
        return wholes[kind].at[pl.ds(start, depth // 2)]

    def own(piece):
        kind, part = divmod(piece, 2)
        depth = shards[kind].shape[0]
        return shards[kind].at[pl.ds(part * (depth // 2), depth // 2)]

    def source(piece, xr, dist):
        return own(piece) if (xr, dist) == (0, 0) else rows(piece, xr, dist, 0)

    sent = []

    def send(copy):
        copy.start()
        sent.append(copy)

    def send_half(piece):
        send(remote(own(piece), rows(piece, 0, 0, 0), half_send.at[piece], ring_recv.at[piece, 1, 0, 0], half))

    def ring_send(piece, xr, dist, sems, dist_there, cr_there, device):
        send(
            remote(
                source(piece, xr, dist),
                rows(piece, xr, dist, 0),
                sems.at[piece, xr, dist],
                ring_recv.at[piece, xr, dist_there, cr_there],
                device,
            )
        )

    def send_plus(piece, xr, dist):
        ring_send(piece, xr, dist, plus_send, dist + 1, 0, z_plus)

    def send_minus(piece, xr, dist):
        ring_send(piece, xr, dist, minus_send, (dist - 1) % zs, 0, z_minus)

    def send_core(piece, xr, dist):
        ring_send(piece, xr, dist, core_send, dist, 1, sibling)

    def arrived(piece, xr, dist, cr):
        ref = rows(piece, xr, dist, cr)
        remote(ref, ref, core_send.at[piece, xr, dist], ring_recv.at[piece, xr, dist, cr], sibling).wait_recv()

    plus = (zs // 2, zs - 1 - zs // 2)
    minus = (zs - 1 - zs // 2, zs // 2)
    steps = zs // 2

    def begin(pieces_here, xr):
        for piece in pieces_here:
            if xr:
                arrived(piece, xr, 0, 0)
            send_plus(piece, xr, 0)
            send_minus(piece, xr, 0)
        for piece in pieces_here:
            send_core(piece, xr, 0)

    def ring_step(pieces_here, step, halves=(0, 1), between=None):
        kind = pieces_here[0] // 2
        for xr in halves:
            for piece in pieces_here:
                if step <= plus[kind]:
                    arrived(piece, xr, step, 0)
                    if step < plus[kind]:
                        send_plus(piece, xr, step)
                    send_core(piece, xr, step)
                if step <= minus[kind]:
                    arrived(piece, xr, zs - step, 0)
                    if step < minus[kind]:
                        send_minus(piece, xr, zs - step)
                    send_core(piece, xr, zs - step)
                if between is not None:
                    between()

    own_columns = pl.ds(pl.multiple_of(core * half_columns, 128), half_columns)
    sibling_columns = pl.ds(pl.multiple_of((1 - core) * half_columns, 128), half_columns)

    def piece_copy(i):
        columns = own_columns if i == 1 else sibling_columns
        device = (sibling, other_z, other_z_sibling)[i]
        return remote(piece_ref.at[:, columns], pieces.at[i], piece_send.at[i], piece_recv.at[i], device)

    def merge_pieces():
        total = piece_ref[:, own_columns].astype(jnp.float32)
        for i in range(3):
            piece_copy(i).wait_recv()
            total = total + pieces[i].astype(jnp.float32)
        policy_tile(0)[...] = total.astype(jnp.bfloat16)

    def skip_copy(i, dz):
        ref = policy_tile(dz)
        return remote(ref, ref, pair_send.at[i], pair_recv.at[i], skip_to[i])

    def send_skips():
        for i in range(len(skips)):
            send(skip_copy(i, 0))

    def policy_to_core(a, b):
        ref = policy_rows(a, b, 0)
        send(remote(ref, ref, policy_core_send.at[a, b], policy_core_recv.at[a, b], sibling))

    part_unit = unit_rows // 2

    def first_copy(i, a):
        ref = policy_rows(a, 0, 0) if i < 2 else policy_rows(a, 0, 0, (i - 2) * part_unit, part_unit)
        return remote(ref, ref, first_send.at[i], first_recv.at[i], (first_plus, first_minus)[i % 2])

    def first_begin():
        for i, dz in enumerate(skips):
            skip_copy(i, zs - dz).wait_recv()
        send(first_copy(0, 0))
        send(first_copy(1, 0))
        policy_to_core(0, 0)

    def first_forward():
        for i, a in ((0, 1), (1, 3)):
            first_copy(i, a).wait_recv()
            send(first_copy(2 + i, a))
            policy_to_core(a, 0)

    def second_copy(a, i, b):
        ref = policy_rows(a, b, 0)
        device = second_plus if i == 0 or (i == 2 and a < 2) else second_minus
        return remote(ref, ref, second_send.at[a, i], second_recv.at[a, i], device)

    def second_begin():
        for i in (2, 3):
            first_copy(i, 2).wait_recv()
        policy_to_core(2, 0)
        for a in range(xs):
            send(second_copy(a, 0, 0))
            send(second_copy(a, 1, 0))

    def second_forward():
        for a in range(xs):
            for i, b in ((0, 1), (1, 3)):
                second_copy(a, i, b).wait_recv()
                if (i == 0) == (a < 2):
                    send(second_copy(a, 2, b))
                policy_to_core(a, b)

    def second_end():
        for a in range(xs):
            second_copy(a, 2, 2).wait_recv()
            policy_to_core(a, 2)

    def fill(k):
        wanted = to_peer[k][0]
        block = pos_ref[0:BLOCK, :]
        for b in range(1, bv_ref.shape[0]):
            block = jnp.where(bv_ref[b] == wanted, pos_ref[b * BLOCK : (b + 1) * BLOCK, :], block)
        if k == local:
            incoming[k] = block
        else:
            outgoing[k] = block

    def dispatch(k):
        send(remote(outgoing.at[k], incoming.at[k], slot_send.at[k], slot_recv.at[k], to_peer[k]))

    rows_here, moves = rows_ref.shape
    place = lax.rem(m, tile_rows // rows_here) * rows_here
    spread = lax.broadcasted_iota(jnp.int32, (tile_rows, rows_here), 0) == place + lax.broadcasted_iota(
        jnp.int32, (tile_rows, rows_here), 1
    )
    piece_ref[...] = jnp.zeros(piece_ref.shape, jnp.bfloat16)
    piece_ref[:, :moves] = jnp.dot(
        spread.astype(jnp.bfloat16), rows_ref[...], preferred_element_type=jnp.float32
    ).astype(jnp.bfloat16)
    for k in range(slots):
        fill(k)

    pl.semaphore_wait(barrier, len(greeted))
    for i in range(3):
        send(piece_copy(i))
    for piece in up_pieces:
        send_half(piece)
    begin(up_pieces, 0)
    for piece in down_pieces:
        send_half(piece)
    begin(down_pieces, 0)

    early = slots // 4
    for k in range(early):
        dispatch(k)

    for kind in range(2):
        depth = shards[kind].shape[0]
        wholes[kind][pl.ds(pl.multiple_of(m * depth, depth), depth), :] = shards[kind][...]

    total_rows = normed.shape[0]
    part_rows = total_rows // 2
    width = 256
    up_parts = 2 * (up_all.shape[1] // width)
    made = []

    def up_part():
        index = len(made)
        if index >= up_parts:
            return
        made.append(index)
        column_rows = pl.ds(index % 2 * part_rows, part_rows)
        columns = pl.ds(index // 2 * width, width)
        upward = jnp.dot(normed[column_rows, :], up_all[:, columns], preferred_element_type=jnp.float32)
        active[column_rows, columns] = jax.nn.gelu(upward, approximate=True).astype(jnp.bfloat16)

    middle = slots // 2
    merge_pieces()
    begin(up_pieces, 1)
    begin(down_pieces, 1)
    send_skips()
    ring_step(up_pieces, 1)
    first_begin()
    for k in range(early, middle):
        dispatch(k)
    ring_step(up_pieces, 2)
    first_forward()
    for k in range(middle, local):
        dispatch(k)
    ring_step(down_pieces, 1, (0,))
    for step in range(3, steps):
        ring_step(up_pieces, step)
    ring_step(down_pieces, 1, (1,))
    second_begin()
    ring_step(up_pieces, steps)
    ring_step(down_pieces, 2)

    for k in range(slots):
        if k != local:
            remote(outgoing.at[k], incoming.at[k], slot_send.at[k], slot_recv.at[k], to_peer[k]).wait_recv()
        normed[pl.ds(k * BLOCK, BLOCK), :] = rms_scale(incoming[k].astype(jnp.float32), ng_ref[...]).astype(
            jnp.bfloat16
        )
    for piece in up_pieces:
        for xr in range(XHI):
            for dist in range(zs):
                arrived(piece, xr, dist, 1)

    for step in range(3, steps):
        ring_step(down_pieces, step, between=up_part)
    for _ in range(up_parts // 2):
        up_part()
    second_forward()
    ring_step(down_pieces, steps, between=up_part)
    for _ in range(up_parts):
        up_part()
    for piece in down_pieces:
        for xr in range(XHI):
            for dist in range(zs):
                arrived(piece, xr, dist, 1)

    def give_back(k):
        send(remote(hidden.at[k], returned.at[k], back_send.at[k], back_recv.at[k], from_peer[k]))
        send(remote(estimate.at[k], estimate_back.at[k], value_send.at[k], value_recv.at[k], from_peer[k]))

    for first in range(0, slots, GROUP):
        downward = jnp.dot(
            active[pl.ds(first * BLOCK, GROUP * BLOCK), :], down_all[...], preferred_element_type=jnp.float32
        )
        for k in range(first, first + GROUP):
            part = downward[(k - first) * BLOCK : (k - first + 1) * BLOCK]
            final = rms_scale(incoming[k].astype(jnp.float32) + part, fg_ref[...])
            kept, kept_value = (returned, estimate_back) if k == local else (hidden, estimate)
            kept[k] = final.astype(jnp.bfloat16)
            value = jnp.tanh(jnp.sum(final * vw_ref[...], axis=-1, keepdims=True))
            kept_value[k] = jnp.transpose(jnp.broadcast_to(value, (BLOCK, BLOCK)))[0:8]
        for k in range(first, first + GROUP):
            if k != local:
                give_back(k)

    second_end()
    for a in range(xs):
        for b in range(ys):
            ref = policy_rows(a, b, 1)
            remote(ref, ref, policy_core_send.at[a, b], policy_core_recv.at[a, b], sibling).wait_recv()

    count = count_ref[0]
    blocks = bv_ref.shape[0]
    games = lax.broadcasted_iota(jnp.int32, (1, BLOCK), 1)
    whole_tiles = moves // width
    rest = moves - whole_tiles * width

    def slot_logits(k, keep, columns, count_rows, row, fresh):
        logits = jnp.dot(returned[k], policy_all[:, columns], preferred_element_type=jnp.float32)
        turned = jnp.transpose(logits.astype(jnp.bfloat16))[:count_rows]
        for b in range(blocks):
            place = (pl.ds(row, count_rows), pl.ds(b * BLOCK, BLOCK))
            part = turned * keep[b]
            policy_out[place] = part if fresh else policy_out[place] + part

    for position, k in enumerate([local, *range(local)]):
        if k != local:
            remote(hidden.at[k], returned.at[k], back_send.at[k], back_recv.at[k], from_peer[k]).wait_recv()
            remote(
                estimate.at[k], estimate_back.at[k], value_send.at[k], value_recv.at[k], from_peer[k]
            ).wait_recv()
        keep = [
            jnp.where((games + b * BLOCK < count) & (bv_ref[b] == to_peer[k][0]), 1.0, 0.0).astype(jnp.bfloat16)
            for b in range(blocks)
        ]

        def step_of(i, carry):
            row = pl.multiple_of(i * width, width)
            slot_logits(k, keep, pl.ds(row, width), width, row, position == 0)
            return carry

        lax.fori_loop(0, whole_tiles, step_of, 0)
        if rest:
            slot_logits(k, keep, pl.ds(whole_tiles * width, width), rest, whole_tiles * width, position == 0)

    for b in range(blocks):
        value = estimate_back[0]
        for k in range(1, slots):
            value = jnp.where(bv_ref[b] == to_peer[k][0], estimate_back[k], value)
        val_out[pl.ds(b, 1), :] = jnp.where(games + b * BLOCK < count, value[0:1], 0.0)

    for copy in sent:
        copy.wait_send()


def local(
    positions,
    game_counts,
    block_variant,
    norm_gain,
    up_weight,
    down_weight,
    final_gain,
    value_weight,
    policy_weight,
):
    variants, members = lax.axis_size("variant"), lax.axis_size("mp")
    zs = members // (XHI * CORES)
    games_here, width = positions.shape
    blocks = block_variant.shape[0]
    up_rows, ffw = up_weight.shape[1:]
    down_rows = down_weight.shape[1]
    slots = variants
    vmem = pl.BlockSpec(memory_space=pltpu.VMEM)
    dma = pltpu.SemaphoreType.DMA
    policy_rows_here, moves = policy_weight.shape
    half_columns = -(-moves // (CORES * 128)) * 128
    tile_rows = 2 * CORES * policy_rows_here
    policy, value = pl.pallas_call(
        functools.partial(exchange_kernel, variants, members),
        out_shape=(
            jax.ShapeDtypeStruct((moves, games_here), jnp.bfloat16),
            jax.ShapeDtypeStruct((blocks, BLOCK), jnp.float32),
        ),
        in_specs=[pl.BlockSpec(memory_space=pltpu.SMEM)]
        + [vmem] * 6
        + [pl.BlockSpec(memory_space=pltpu.SMEM), vmem],
        out_specs=(vmem, vmem),
        scratch_shapes=[
            pltpu.VMEM((slots, BLOCK, width), jnp.bfloat16),
            pltpu.VMEM((slots, BLOCK, width), jnp.bfloat16),
            pltpu.VMEM((slots * BLOCK, width), jnp.bfloat16),
            pltpu.VMEM((slots * BLOCK, ffw), jnp.bfloat16),
            pltpu.VMEM((up_rows * members, ffw), jnp.bfloat16),
            pltpu.VMEM((down_rows * members, width), jnp.bfloat16),
            pltpu.VMEM((slots, BLOCK, width), jnp.bfloat16),
            pltpu.VMEM((slots, BLOCK, width), jnp.bfloat16),
            pltpu.VMEM((slots, 8, BLOCK), jnp.float32),
            pltpu.VMEM((slots, 8, BLOCK), jnp.float32),
            dma((4, XHI, zs, CORES)),
            dma((4, XHI, zs)),
            dma((4, XHI, zs)),
            dma((4, XHI, zs)),
            dma((4,)),
            dma((slots,)),
            dma((slots,)),
            dma((slots,)),
            dma((slots,)),
            dma((slots,)),
            dma((slots,)),
            pltpu.VMEM((tile_rows, CORES * half_columns), jnp.bfloat16),
            pltpu.VMEM((variants * members * policy_rows_here, CORES * half_columns), jnp.bfloat16),
            pltpu.VMEM((3, tile_rows, half_columns), jnp.bfloat16),
            dma((3,)),
            dma((3,)),
            dma((3,)),
            dma((3,)),
            dma((4,)),
            dma((4,)),
            dma((4, 3)),
            dma((4, 3)),
            dma((4, 4)),
            dma((4, 4)),
        ],
        compiler_params=pltpu.CompilerParams(
            collective_id=0, has_side_effects=True, vmem_limit_bytes=58 * 1024 * 1024
        ),
        cost_estimate=pl.CostEstimate(
            flops=4 * slots * BLOCK * width * ffw, bytes_accessed=4 * width * ffw, transcendentals=0
        ),
        name="exchange",
    )(
        block_variant,
        positions,
        up_weight[0],
        down_weight[0],
        norm_gain,
        final_gain,
        value_weight,
        game_counts,
        policy_weight,
    )
    return (policy.T, value.reshape(games_here))


def solution(mesh):
    in_specs = (
        P(("variant", "mp"), None),
        P(("variant", "mp")),
        P(("variant", "mp")),
        P("variant", None),
        P("variant", "mp", None),
        P("variant", "mp", None),
        P("variant", None),
        P("variant", None),
        P(("variant", "mp"), None),
    )
    out_specs = (P(("variant", "mp"), None), P(("variant", "mp")))
    return jax.shard_map(local, mesh=mesh, in_specs=in_specs, out_specs=out_specs, check_vma=False)
```

```python
import functools

import jax
import jax.numpy as jnp
from jax import lax
from jax.experimental import pallas as pl
from jax.experimental.pallas import tpu as pltpu
from jax.sharding import PartitionSpec as P

MESH = pl.DeviceIdType.MESH
BLOCK = 128
EPS = 1e-06
XLO, XHI, CORES = 2, 2, 2
GROUP = 2


def rms_scale(values, gain):
    mean_square = jnp.mean(values * values, axis=-1, keepdims=True)
    return values * lax.rsqrt(mean_square + EPS) * gain


def remote(src, dst, send_sem, recv_sem, device):
    return pltpu.make_async_remote_copy(
        src_ref=src, dst_ref=dst, send_sem=send_sem, recv_sem=recv_sem, device_id=device, device_id_type=MESH
    )


def exchange_kernel(
    variants,
    members,
    bv_ref,
    pos_ref,
    up_ref,
    down_ref,
    ng_ref,
    fg_ref,
    vw_ref,
    count_ref,
    rows_ref,
    policy_out,
    val_out,
    outgoing,
    incoming,
    normed,
    active,
    up_all,
    down_all,
    hidden,
    returned,
    estimate,
    estimate_back,
    ring_recv,
    plus_send,
    minus_send,
    core_send,
    half_send,
    slot_send,
    slot_recv,
    back_send,
    back_recv,
    value_send,
    value_recv,
    own_hidden,
    piece_ref,
    policy_all,
    pieces,
    piece_send,
    piece_recv,
    pair_send,
    pair_recv,
    first_send,
    first_recv,
    second_send,
    second_recv,
    policy_core_send,
    policy_core_recv,
):
    ys, zs = variants // XLO, members // (XHI * CORES)
    v, m = lax.axis_index("variant"), lax.axis_index("mp")
    y, xl = lax.div(v, XLO), lax.rem(v, XLO)
    xh, z, core = lax.div(m, zs * CORES), lax.rem(lax.div(m, CORES), zs), lax.rem(m, CORES)

    def member(xr, dz, cr):
        return (lax.rem(xh + xr, XHI) * zs + lax.rem(z + dz, zs)) * CORES + lax.rem(core + cr, CORES)

    def peer(dy, dx):
        return lax.rem(y + dy, ys) * XLO + lax.rem(xl + dx, XLO)

    z_plus, z_minus = (v, member(0, 1, 0)), (v, member(0, zs - 1, 0))
    sibling, half = (v, member(0, 0, 1)), (v, member(1, 0, 0))
    order = sorted(
        ((dy, dx) for dy in range(ys) for dx in range(XLO)), key=lambda r: (-min(r[0], ys - r[0]), -r[1])
    )
    to_peer = [(peer(dy, dx), m) for dy, dx in order]
    from_peer = [(peer(ys - dy, XLO - dx), m) for dy, dx in order]
    slots = len(order)
    local = slots - 1

    half_columns = policy_all.shape[1] // CORES
    tile_rows = piece_ref.shape[0]
    unit_rows = zs // 2 * tile_rows
    paired = z + 1 - 2 * lax.rem(z, 2) - z
    other_z = (v, member(0, zs + paired, 0))
    x = xh * XLO + xl
    xs = XHI * XLO

    def chip(cx, cy):
        cx, cy = lax.rem(cx, xs), lax.rem(cy, ys)
        return cy * XLO + lax.rem(cx, XLO), (lax.div(cx, XLO) * zs + z) * CORES + core

    def along(first, second):
        return x + first * (1 - core) + second * core, y + first * core + second * (1 - core)

    first_plus, first_minus = chip(*along(1, 0)), chip(*along(3, 0))
    second_plus, second_minus = chip(*along(0, 1)), chip(*along(0, 3))
    out_z = (v, member(0, zs - paired, 0))

    def policy_rows(a, b, cr, start=0, count=None):
        axis = lax.rem(core + cr, CORES)
        cx = lax.rem(x + (xs - a) * (1 - axis) + (xs - b) * axis, xs)
        cy = lax.rem(y + (ys - a) * axis + (ys - b) * (1 - axis), ys)
        group = (cy * XLO + lax.rem(cx, XLO)) * XHI + lax.div(cx, XLO)
        row = pl.multiple_of(group * unit_rows + start, tile_rows)
        column = pl.multiple_of(axis * half_columns, 128)
        return policy_all.at[pl.ds(row, unit_rows if count is None else count), pl.ds(column, half_columns)]

    def policy_tile(dz):
        return policy_rows(0, 0, 0, lax.div(lax.rem(z + dz, zs), 2) * tile_rows, tile_rows)

    barrier = pltpu.get_barrier_semaphore()
    greeted = [z_plus, z_minus, sibling, half, *to_peer[:local], (peer(0, 1), member(1, 0, 0))]
    for device in greeted:
        pl.semaphore_signal(barrier, inc=1, device_id=device, device_id_type=MESH)

    shards, wholes = (up_ref, down_ref), (up_all, down_all)

    up_pieces, down_pieces = (0, 1), (2, 3)

    def rows(piece, xr, dist, cr):
        kind, part = divmod(piece, 2)
        depth = shards[kind].shape[0]
        owner = member(xr, zs - dist, cr)
        start = pl.multiple_of(owner * depth + part * (depth // 2), depth // 2)
        return wholes[kind].at[pl.ds(start, depth // 2)]

    def own(piece):
        kind, part = divmod(piece, 2)
        depth = shards[kind].shape[0]
        return shards[kind].at[pl.ds(part * (depth // 2), depth // 2)]

    def source(piece, xr, dist):
        return own(piece) if (xr, dist) == (0, 0) else rows(piece, xr, dist, 0)

    sent = []

    def send(copy):
        copy.start()
        sent.append(copy)

    def send_half(piece):
        send(remote(own(piece), rows(piece, 0, 0, 0), half_send.at[piece], ring_recv.at[piece, 1, 0, 0], half))

    def ring_send(piece, xr, dist, sems, dist_there, cr_there, device):
        send(
            remote(
                source(piece, xr, dist),
                rows(piece, xr, dist, 0),
                sems.at[piece, xr, dist],
                ring_recv.at[piece, xr, dist_there, cr_there],
                device,
            )
        )

    def send_plus(piece, xr, dist):
        ring_send(piece, xr, dist, plus_send, dist + 1, 0, z_plus)

    def send_minus(piece, xr, dist):
        ring_send(piece, xr, dist, minus_send, (dist - 1) % zs, 0, z_minus)

    def send_core(piece, xr, dist):
        ring_send(piece, xr, dist, core_send, dist, 1, sibling)

    def arrived(piece, xr, dist, cr):
        ref = rows(piece, xr, dist, cr)
        remote(ref, ref, core_send.at[piece, xr, dist], ring_recv.at[piece, xr, dist, cr], sibling).wait_recv()

    plus = (zs // 2, zs - 1 - zs // 2)
    minus = (zs - 1 - zs // 2, zs // 2)
    steps = zs // 2

    def begin(pieces_here, xr):
        for piece in pieces_here:
            if xr:
                arrived(piece, xr, 0, 0)
            send_plus(piece, xr, 0)
            send_minus(piece, xr, 0)
        for piece in pieces_here:
            send_core(piece, xr, 0)

    def ring_step(pieces_here, step, halves=(0, 1), between=None):
        kind = pieces_here[0] // 2
        for xr in halves:
            for piece in pieces_here:
                if step <= plus[kind]:
                    arrived(piece, xr, step, 0)
                    if step < plus[kind]:
                        send_plus(piece, xr, step)
                    send_core(piece, xr, step)
                if step <= minus[kind]:
                    arrived(piece, xr, zs - step, 0)
                    if step < minus[kind]:
                        send_minus(piece, xr, zs - step)
                    send_core(piece, xr, zs - step)
                if between is not None:
                    between()

    own_columns = pl.ds(pl.multiple_of(core * half_columns, 128), half_columns)
    sibling_columns = pl.ds(pl.multiple_of((1 - core) * half_columns, 128), half_columns)

    def piece_copy(i):
        source_ref = piece_ref.at[:, sibling_columns] if i == 0 else pieces.at[2]
        return remote(source_ref, pieces.at[i], piece_send.at[i], piece_recv.at[i], (sibling, other_z)[i])

    def merge_chip():
        piece_copy(0).wait_recv()
        mine = piece_ref[:, own_columns].astype(jnp.float32)
        pieces[2] = (mine + pieces[0].astype(jnp.float32)).astype(jnp.bfloat16)

    def merge_pair():
        piece_copy(1).wait_recv()
        total = pieces[2].astype(jnp.float32) + pieces[1].astype(jnp.float32)
        policy_tile(0)[...] = total.astype(jnp.bfloat16)

    hop_sent = (0, zs - paired, 2 * zs + 2 * paired)
    hop_got = (zs - paired, 2 * zs + 2 * paired, 3 * zs - 3 * paired)

    def hop_copy(i, dz):
        ref = policy_tile(dz)
        return remote(ref, ref, pair_send.at[i], pair_recv.at[i], (out_z, other_z, out_z)[i])

    def hop_send(i):
        if i:
            hop_copy(i - 1, hop_got[i - 1]).wait_recv()
        send(hop_copy(i, hop_sent[i]))

    def policy_to_core(a, b):
        ref = policy_rows(a, b, 0)
        send(remote(ref, ref, policy_core_send.at[a, b], policy_core_recv.at[a, b], sibling))

    part_unit = unit_rows // 2

    def first_copy(i, a):
        ref = policy_rows(a, 0, 0) if i < 2 else policy_rows(a, 0, 0, (i - 2) * part_unit, part_unit)
        return remote(ref, ref, first_send.at[i], first_recv.at[i], (first_plus, first_minus)[i % 2])

    def first_begin():
        hop_copy(2, hop_got[2]).wait_recv()
        send(first_copy(0, 0))
        send(first_copy(1, 0))
        policy_to_core(0, 0)

    def first_forward():
        for i, a in ((0, 1), (1, 3)):
            first_copy(i, a).wait_recv()
            send(first_copy(2 + i, a))
            policy_to_core(a, 0)

    def second_copy(a, i, b):
        ref = policy_rows(a, b, 0)
        device = second_plus if i == 0 or (i == 2 and a < 2) else second_minus
        return remote(ref, ref, second_send.at[a, i], second_recv.at[a, i], device)

    def second_begin():
        for i in (2, 3):
            first_copy(i, 2).wait_recv()
        policy_to_core(2, 0)
        for a in range(xs):
            send(second_copy(a, 0, 0))
            send(second_copy(a, 1, 0))

    def second_forward():
        for a in range(xs):
            for i, b in ((0, 1), (1, 3)):
                second_copy(a, i, b).wait_recv()
                if (i == 0) == (a < 2):
                    send(second_copy(a, 2, b))
                policy_to_core(a, b)

    def second_end():
        for a in range(xs):
            second_copy(a, 2, 2).wait_recv()
            policy_to_core(a, 2)

    def fill(k):
        wanted = to_peer[k][0]
        block = pos_ref[0:BLOCK, :]
        for b in range(1, bv_ref.shape[0]):
            block = jnp.where(bv_ref[b] == wanted, pos_ref[b * BLOCK : (b + 1) * BLOCK, :], block)
        if k == local:
            incoming[k] = block
        else:
            outgoing[k] = block

    def dispatch(k):
        send(remote(outgoing.at[k], incoming.at[k], slot_send.at[k], slot_recv.at[k], to_peer[k]))

    rows_here, moves = rows_ref.shape
    place = lax.rem(m, tile_rows // rows_here) * rows_here
    spread = lax.broadcasted_iota(jnp.int32, (tile_rows, rows_here), 0) == place + lax.broadcasted_iota(
        jnp.int32, (tile_rows, rows_here), 1
    )
    piece_ref[...] = jnp.zeros(piece_ref.shape, jnp.bfloat16)
    piece_ref[:, :moves] = jnp.dot(
        spread.astype(jnp.bfloat16), rows_ref[...], preferred_element_type=jnp.float32
    ).astype(jnp.bfloat16)
    for k in range(slots):
        fill(k)

    pl.semaphore_wait(barrier, len(greeted))
    send(piece_copy(0))
    for piece in (*up_pieces, *down_pieces):
        send_half(piece)
    begin(up_pieces, 0)
    for k in range(local):
        dispatch(k)
    merge_chip()

    for kind in range(2):
        depth = shards[kind].shape[0]
        wholes[kind][pl.ds(pl.multiple_of(m * depth, depth), depth), :] = shards[kind][...]

    send(piece_copy(1))
    begin(down_pieces, 0)

    total_rows = normed.shape[0]
    part_rows = total_rows // 2
    width = 256
    up_parts = 2 * (up_all.shape[1] // width)
    made = []

    def up_part():
        index = len(made)
        if index >= up_parts:
            return
        made.append(index)
        column_rows = pl.ds(index % 2 * part_rows, part_rows)
        columns = pl.ds(index // 2 * width, width)
        upward = jnp.dot(normed[column_rows, :], up_all[:, columns], preferred_element_type=jnp.float32)
        active[column_rows, columns] = jax.nn.gelu(upward, approximate=True).astype(jnp.bfloat16)

    begin(up_pieces, 1)
    merge_pair()
    begin(down_pieces, 1)
    hop_send(0)
    ring_step(up_pieces, 1)
    ring_step(down_pieces, 1, (0,))
    hop_send(1)
    ring_step(up_pieces, 2)
    hop_send(2)
    for step in range(3, steps):
        ring_step(up_pieces, step)
    ring_step(down_pieces, 1, (1,))
    first_begin()
    ring_step(up_pieces, steps)
    ring_step(down_pieces, 2, (0,))
    first_forward()
    ring_step(down_pieces, 2, (1,))

    for k in range(slots):
        if k != local:
            remote(outgoing.at[k], incoming.at[k], slot_send.at[k], slot_recv.at[k], to_peer[k]).wait_recv()
        normed[pl.ds(k * BLOCK, BLOCK), :] = rms_scale(incoming[k].astype(jnp.float32), ng_ref[...]).astype(
            jnp.bfloat16
        )
    for piece in up_pieces:
        for xr in range(XHI):
            for dist in range(zs):
                arrived(piece, xr, dist, 1)

    ring_step(down_pieces, 3, (0,), up_part)
    second_begin()
    ring_step(down_pieces, 3, (1,), up_part)
    for step in range(4, steps):
        ring_step(down_pieces, step, between=up_part)
    for _ in range(up_parts // 2):
        up_part()
    ring_step(down_pieces, steps, between=up_part)
    for _ in range(up_parts):
        up_part()
    for piece in down_pieces:
        for xr in range(XHI):
            for dist in range(zs):
                arrived(piece, xr, dist, 1)

    def give_back(k):
        send(remote(hidden.at[k], returned.at[k], back_send.at[k], back_recv.at[k], from_peer[k]))
        send(remote(estimate.at[k], estimate_back.at[k], value_send.at[k], value_recv.at[k], from_peer[k]))

    for first in range(0, slots, GROUP):
        downward = jnp.dot(
            active[pl.ds(first * BLOCK, GROUP * BLOCK), :], down_all[...], preferred_element_type=jnp.float32
        )
        for k in range(first, first + GROUP):
            part = downward[(k - first) * BLOCK : (k - first + 1) * BLOCK]
            final = rms_scale(incoming[k].astype(jnp.float32) + part, fg_ref[...])
            kept, kept_value = (returned, estimate_back) if k == local else (hidden, estimate)
            kept[k] = final.astype(jnp.bfloat16)
            value = jnp.tanh(jnp.sum(final * vw_ref[...], axis=-1, keepdims=True))
            kept_value[k] = jnp.transpose(jnp.broadcast_to(value, (BLOCK, BLOCK)))[0:8]
        for k in range(first, first + GROUP):
            if k != local:
                give_back(k)
        if first == 0:
            second_forward()

    second_end()
    for k in range(slots):
        if k != local:
            remote(hidden.at[k], returned.at[k], back_send.at[k], back_recv.at[k], from_peer[k]).wait_recv()
            remote(
                estimate.at[k], estimate_back.at[k], value_send.at[k], value_recv.at[k], from_peer[k]
            ).wait_recv()
    for a in range(xs):
        for b in range(ys):
            ref = policy_rows(a, b, 1)
            remote(ref, ref, policy_core_send.at[a, b], policy_core_recv.at[a, b], sibling).wait_recv()

    count = count_ref[0]
    for b in range(bv_ref.shape[0]):
        block, value = returned[0], estimate_back[0]
        for k in range(1, slots):
            chosen = bv_ref[b] == to_peer[k][0]
            block = jnp.where(chosen, returned[k], block)
            value = jnp.where(chosen, estimate_back[k], value)
        own_hidden[pl.ds(b * BLOCK, BLOCK), :] = block
        games = b * BLOCK + lax.broadcasted_iota(jnp.int32, (1, BLOCK), 1)
        val_out[pl.ds(b, 1), :] = jnp.where(games < count, value[0:1], 0.0)

    games_here = policy_out.shape[0]
    live = lax.broadcasted_iota(jnp.int32, (games_here, 1), 0) < count

    def masked_logits(columns):
        logits = jnp.dot(own_hidden[...], policy_all[:, columns], preferred_element_type=jnp.float32)
        return jnp.where(live, logits, 0.0).astype(jnp.bfloat16)

    whole_tiles = moves // width

    def policy_tile_step(i, carry):
        columns = pl.ds(pl.multiple_of(i * width, width), width)
        policy_out[:, columns] = masked_logits(columns)
        return carry

    lax.fori_loop(0, whole_tiles, policy_tile_step, 0)
    rest = moves - whole_tiles * width
    if rest:
        policy_out[:, pl.ds(whole_tiles * width, rest)] = masked_logits(pl.ds(whole_tiles * width, width))[:, :rest]

    for copy in sent:
        copy.wait_send()


def local(
    positions,
    game_counts,
    block_variant,
    norm_gain,
    up_weight,
    down_weight,
    final_gain,
    value_weight,
    policy_weight,
):
    variants, members = lax.axis_size("variant"), lax.axis_size("mp")
    zs = members // (XHI * CORES)
    games_here, width = positions.shape
    blocks = block_variant.shape[0]
    up_rows, ffw = up_weight.shape[1:]
    down_rows = down_weight.shape[1]
    slots = variants
    vmem = pl.BlockSpec(memory_space=pltpu.VMEM)
    dma = pltpu.SemaphoreType.DMA
    policy_rows_here, moves = policy_weight.shape
    half_columns = -(-moves // (CORES * 128)) * 128
    tile_rows = 2 * CORES * policy_rows_here
    policy, value = pl.pallas_call(
        functools.partial(exchange_kernel, variants, members),
        out_shape=(
            jax.ShapeDtypeStruct((games_here, moves), jnp.bfloat16),
            jax.ShapeDtypeStruct((blocks, BLOCK), jnp.float32),
        ),
        in_specs=[pl.BlockSpec(memory_space=pltpu.SMEM)]
        + [vmem] * 6
        + [pl.BlockSpec(memory_space=pltpu.SMEM), vmem],
        out_specs=(vmem, vmem),
        scratch_shapes=[
            pltpu.VMEM((slots, BLOCK, width), jnp.bfloat16),
            pltpu.VMEM((slots, BLOCK, width), jnp.bfloat16),
            pltpu.VMEM((slots * BLOCK, width), jnp.bfloat16),
            pltpu.VMEM((slots * BLOCK, ffw), jnp.bfloat16),
            pltpu.VMEM((up_rows * members, ffw), jnp.bfloat16),
            pltpu.VMEM((down_rows * members, width), jnp.bfloat16),
            pltpu.VMEM((slots, BLOCK, width), jnp.bfloat16),
            pltpu.VMEM((slots, BLOCK, width), jnp.bfloat16),
            pltpu.VMEM((slots, 8, BLOCK), jnp.float32),
            pltpu.VMEM((slots, 8, BLOCK), jnp.float32),
            dma((4, XHI, zs, CORES)),
            dma((4, XHI, zs)),
            dma((4, XHI, zs)),
            dma((4, XHI, zs)),
            dma((4,)),
            dma((slots,)),
            dma((slots,)),
            dma((slots,)),
            dma((slots,)),
            dma((slots,)),
            dma((slots,)),
            pltpu.VMEM((games_here, width), jnp.bfloat16),
            pltpu.VMEM((tile_rows, CORES * half_columns), jnp.bfloat16),
            pltpu.VMEM((variants * members * policy_rows_here, CORES * half_columns), jnp.bfloat16),
            pltpu.VMEM((3, tile_rows, half_columns), jnp.bfloat16),
            dma((3,)),
            dma((3,)),
            dma((3,)),
            dma((3,)),
            dma((4,)),
            dma((4,)),
            dma((4, 3)),
            dma((4, 3)),
            dma((4, 4)),
            dma((4, 4)),
        ],
        compiler_params=pltpu.CompilerParams(
            collective_id=0, has_side_effects=True, vmem_limit_bytes=58 * 1024 * 1024
        ),
        cost_estimate=pl.CostEstimate(
            flops=4 * slots * BLOCK * width * ffw, bytes_accessed=4 * width * ffw, transcendentals=0
        ),
        name="exchange",
    )(
        block_variant,
        positions,
        up_weight[0],
        down_weight[0],
        norm_gain,
        final_gain,
        value_weight,
        game_counts,
        policy_weight,
    )
    return (policy, value.reshape(games_here))


def solution(mesh):
    in_specs = (
        P(("variant", "mp"), None),
        P(("variant", "mp")),
        P(("variant", "mp")),
        P("variant", None),
        P("variant", "mp", None),
        P("variant", "mp", None),
        P("variant", None),
        P("variant", None),
        P(("variant", "mp"), None),
    )
    out_specs = (P(("variant", "mp"), None), P(("variant", "mp")))
    return jax.shard_map(local, mesh=mesh, in_specs=in_specs, out_specs=out_specs, check_vma=False)
```

```python
import functools

import jax
import jax.numpy as jnp
from jax import lax
from jax.experimental import pallas as pl
from jax.experimental.pallas import tpu as pltpu
from jax.sharding import PartitionSpec as P

MESH = pl.DeviceIdType.MESH
BLOCK = 128
EPS = 1e-06
XLO, XHI, CORES = 2, 2, 2
GROUP = 2


def rms_scale(values, gain):
    mean_square = jnp.mean(values * values, axis=-1, keepdims=True)
    return values * lax.rsqrt(mean_square + EPS) * gain


def remote(src, dst, send_sem, recv_sem, device):
    return pltpu.make_async_remote_copy(
        src_ref=src, dst_ref=dst, send_sem=send_sem, recv_sem=recv_sem, device_id=device, device_id_type=MESH
    )


def exchange_kernel(
    variants,
    members,
    bv_ref,
    pos_ref,
    up_ref,
    down_ref,
    ng_ref,
    fg_ref,
    vw_ref,
    count_ref,
    rows_ref,
    policy_out,
    val_out,
    outgoing,
    incoming,
    normed,
    active,
    up_all,
    down_all,
    hidden,
    returned,
    estimate,
    estimate_back,
    ring_recv,
    plus_send,
    minus_send,
    core_send,
    half_send,
    slot_send,
    slot_recv,
    back_send,
    back_recv,
    value_send,
    value_recv,
    own_hidden,
    piece_ref,
    policy_all,
    pieces,
    piece_send,
    piece_recv,
    pair_send,
    pair_recv,
    first_send,
    first_recv,
    second_send,
    second_recv,
    policy_core_send,
    policy_core_recv,
):
    ys, zs = variants // XLO, members // (XHI * CORES)
    v, m = lax.axis_index("variant"), lax.axis_index("mp")
    y, xl = lax.div(v, XLO), lax.rem(v, XLO)
    xh, z, core = lax.div(m, zs * CORES), lax.rem(lax.div(m, CORES), zs), lax.rem(m, CORES)

    def member(xr, dz, cr):
        return (lax.rem(xh + xr, XHI) * zs + lax.rem(z + dz, zs)) * CORES + lax.rem(core + cr, CORES)

    def peer(dy, dx):
        return lax.rem(y + dy, ys) * XLO + lax.rem(xl + dx, XLO)

    z_plus, z_minus = (v, member(0, 1, 0)), (v, member(0, zs - 1, 0))
    sibling, half = (v, member(0, 0, 1)), (v, member(1, 0, 0))
    order = sorted(
        ((dy, dx) for dy in range(ys) for dx in range(XLO)), key=lambda r: (-min(r[0], ys - r[0]), -r[1])
    )
    to_peer = [(peer(dy, dx), m) for dy, dx in order]
    from_peer = [(peer(ys - dy, XLO - dx), m) for dy, dx in order]
    slots = len(order)
    local = slots - 1

    half_columns = policy_all.shape[1] // CORES
    tile_rows = piece_ref.shape[0]
    unit_rows = zs // 2 * tile_rows
    paired = z + 1 - 2 * lax.rem(z, 2) - z
    other_z = (v, member(0, zs + paired, 0))
    x = xh * XLO + xl
    xs = XHI * XLO

    def chip(cx, cy):
        cx, cy = lax.rem(cx, xs), lax.rem(cy, ys)
        return cy * XLO + lax.rem(cx, XLO), (lax.div(cx, XLO) * zs + z) * CORES + core

    def along(first, second):
        return x + first * (1 - core) + second * core, y + first * core + second * (1 - core)

    first_plus, first_minus = chip(*along(1, 0)), chip(*along(3, 0))
    second_plus, second_minus = chip(*along(0, 1)), chip(*along(0, 3))
    out_z = (v, member(0, zs - paired, 0))

    def policy_rows(a, b, cr, start=0, count=None):
        axis = lax.rem(core + cr, CORES)
        cx = lax.rem(x + (xs - a) * (1 - axis) + (xs - b) * axis, xs)
        cy = lax.rem(y + (ys - a) * axis + (ys - b) * (1 - axis), ys)
        group = (cy * XLO + lax.rem(cx, XLO)) * XHI + lax.div(cx, XLO)
        row = pl.multiple_of(group * unit_rows + start, tile_rows)
        column = pl.multiple_of(axis * half_columns, 128)
        return policy_all.at[pl.ds(row, unit_rows if count is None else count), pl.ds(column, half_columns)]

    def policy_tile(dz):
        return policy_rows(0, 0, 0, lax.div(lax.rem(z + dz, zs), 2) * tile_rows, tile_rows)

    barrier = pltpu.get_barrier_semaphore()
    greeted = [z_plus, z_minus, sibling, half, *to_peer[:local], (peer(0, 1), member(1, 0, 0))]
    for device in greeted:
        pl.semaphore_signal(barrier, inc=1, device_id=device, device_id_type=MESH)

    shards, wholes = (up_ref, down_ref), (up_all, down_all)

    up_pieces, down_pieces = (0, 1), (2, 3)

    def rows(piece, xr, dist, cr):
        kind, part = divmod(piece, 2)
        depth = shards[kind].shape[0]
        owner = member(xr, zs - dist, cr)
        start = pl.multiple_of(owner * depth + part * (depth // 2), depth // 2)
        return wholes[kind].at[pl.ds(start, depth // 2)]

    def own(piece):
        kind, part = divmod(piece, 2)
        depth = shards[kind].shape[0]
        return shards[kind].at[pl.ds(part * (depth // 2), depth // 2)]

    def source(piece, xr, dist):
        return own(piece) if (xr, dist) == (0, 0) else rows(piece, xr, dist, 0)

    sent = []

    def send(copy):
        copy.start()
        sent.append(copy)

    def send_half(piece):
        send(remote(own(piece), rows(piece, 0, 0, 0), half_send.at[piece], ring_recv.at[piece, 1, 0, 0], half))

    def ring_send(piece, xr, dist, sems, dist_there, cr_there, device):
        send(
            remote(
                source(piece, xr, dist),
                rows(piece, xr, dist, 0),
                sems.at[piece, xr, dist],
                ring_recv.at[piece, xr, dist_there, cr_there],
                device,
            )
        )

    def send_plus(piece, xr, dist):
        ring_send(piece, xr, dist, plus_send, dist + 1, 0, z_plus)

    def send_minus(piece, xr, dist):
        ring_send(piece, xr, dist, minus_send, (dist - 1) % zs, 0, z_minus)

    def send_core(piece, xr, dist):
        ring_send(piece, xr, dist, core_send, dist, 1, sibling)

    def arrived(piece, xr, dist, cr):
        ref = rows(piece, xr, dist, cr)
        remote(ref, ref, core_send.at[piece, xr, dist], ring_recv.at[piece, xr, dist, cr], sibling).wait_recv()

    plus = (zs // 2, zs - 1 - zs // 2)
    minus = (zs - 1 - zs // 2, zs // 2)
    steps = zs // 2

    def begin(pieces_here, xr):
        for piece in pieces_here:
            if xr:
                arrived(piece, xr, 0, 0)
            send_plus(piece, xr, 0)
            send_minus(piece, xr, 0)
        for piece in pieces_here:
            send_core(piece, xr, 0)

    def ring_step(pieces_here, step, halves=(0, 1), between=None):
        kind = pieces_here[0] // 2
        for xr in halves:
            for piece in pieces_here:
                if step <= plus[kind]:
                    arrived(piece, xr, step, 0)
                    if step < plus[kind]:
                        send_plus(piece, xr, step)
                    send_core(piece, xr, step)
                if step <= minus[kind]:
                    arrived(piece, xr, zs - step, 0)
                    if step < minus[kind]:
                        send_minus(piece, xr, zs - step)
                    send_core(piece, xr, zs - step)
                if between is not None:
                    between()

    own_columns = pl.ds(pl.multiple_of(core * half_columns, 128), half_columns)
    sibling_columns = pl.ds(pl.multiple_of((1 - core) * half_columns, 128), half_columns)

    def piece_copy(i):
        source_ref = piece_ref.at[:, sibling_columns] if i == 0 else pieces.at[2]
        return remote(source_ref, pieces.at[i], piece_send.at[i], piece_recv.at[i], (sibling, other_z)[i])

    def merge_chip():
        piece_copy(0).wait_recv()
        mine = piece_ref[:, own_columns].astype(jnp.float32)
        pieces[2] = (mine + pieces[0].astype(jnp.float32)).astype(jnp.bfloat16)

    def merge_pair():
        piece_copy(1).wait_recv()
        total = pieces[2].astype(jnp.float32) + pieces[1].astype(jnp.float32)
        policy_tile(0)[...] = total.astype(jnp.bfloat16)

    hop_sent = (0, zs - paired, 2 * zs + 2 * paired)
    hop_got = (zs - paired, 2 * zs + 2 * paired, 3 * zs - 3 * paired)

    def hop_copy(i, dz):
        ref = policy_tile(dz)
        return remote(ref, ref, pair_send.at[i], pair_recv.at[i], (out_z, other_z, out_z)[i])

    def hop_send(i):
        if i:
            hop_copy(i - 1, hop_got[i - 1]).wait_recv()
        send(hop_copy(i, hop_sent[i]))

    def policy_to_core(a, b):
        ref = policy_rows(a, b, 0)
        send(remote(ref, ref, policy_core_send.at[a, b], policy_core_recv.at[a, b], sibling))

    part_unit = unit_rows // 2

    def first_copy(i, a):
        ref = policy_rows(a, 0, 0) if i < 2 else policy_rows(a, 0, 0, (i - 2) * part_unit, part_unit)
        return remote(ref, ref, first_send.at[i], first_recv.at[i], (first_plus, first_minus)[i % 2])

    def first_begin():
        hop_copy(2, hop_got[2]).wait_recv()
        send(first_copy(0, 0))
        send(first_copy(1, 0))
        second_send_rows(0)
        policy_to_core(0, 0)

    def first_forward():
        for i, a in ((0, 1), (1, 3)):
            first_copy(i, a).wait_recv()
            send(first_copy(2 + i, a))
            second_send_rows(a)
            policy_to_core(a, 0)

    def second_copy(a, i, b):
        ref = policy_rows(a, b, 0)
        device = second_plus if i == 0 or (i == 2 and a < 2) else second_minus
        return remote(ref, ref, second_send.at[a, i], second_recv.at[a, i], device)

    def second_begin():
        for i in (2, 3):
            first_copy(i, 2).wait_recv()
        second_send_rows(2)
        policy_to_core(2, 0)

    def second_send_rows(a):
        send(second_copy(a, 0, 0))
        send(second_copy(a, 1, 0))

    def second_forward():
        for a in range(xs):
            for i, b in ((0, 1), (1, 3)):
                second_copy(a, i, b).wait_recv()
                if (i == 0) == (a < 2):
                    send(second_copy(a, 2, b))
                policy_to_core(a, b)

    def second_end():
        for a in range(xs):
            second_copy(a, 2, 2).wait_recv()
            policy_to_core(a, 2)

    def fill(k):
        wanted = to_peer[k][0]
        block = pos_ref[0:BLOCK, :]
        for b in range(1, bv_ref.shape[0]):
            block = jnp.where(bv_ref[b] == wanted, pos_ref[b * BLOCK : (b + 1) * BLOCK, :], block)
        if k == local:
            incoming[k] = block
        else:
            outgoing[k] = block

    def dispatch(k):
        send(remote(outgoing.at[k], incoming.at[k], slot_send.at[k], slot_recv.at[k], to_peer[k]))

    rows_here, moves = rows_ref.shape
    place = lax.rem(m, tile_rows // rows_here) * rows_here
    spread = lax.broadcasted_iota(jnp.int32, (tile_rows, rows_here), 0) == place + lax.broadcasted_iota(
        jnp.int32, (tile_rows, rows_here), 1
    )
    piece_ref[...] = jnp.zeros(piece_ref.shape, jnp.bfloat16)
    piece_ref[:, :moves] = jnp.dot(
        spread.astype(jnp.bfloat16), rows_ref[...], preferred_element_type=jnp.float32
    ).astype(jnp.bfloat16)
    for k in range(slots):
        fill(k)

    pl.semaphore_wait(barrier, len(greeted))
    send(piece_copy(0))
    for piece in (*up_pieces, *down_pieces):
        send_half(piece)
    begin(up_pieces, 0)
    for k in range(local):
        dispatch(k)
    merge_chip()

    for kind in range(2):
        depth = shards[kind].shape[0]
        wholes[kind][pl.ds(pl.multiple_of(m * depth, depth), depth), :] = shards[kind][...]

    send(piece_copy(1))
    begin(down_pieces, 0)

    total_rows = normed.shape[0]
    part_rows = total_rows // 2
    width = 256
    up_parts = 2 * (up_all.shape[1] // width)
    made = []

    def up_part():
        index = len(made)
        if index >= up_parts:
            return
        made.append(index)
        column_rows = pl.ds(index % 2 * part_rows, part_rows)
        columns = pl.ds(index // 2 * width, width)
        upward = jnp.dot(normed[column_rows, :], up_all[:, columns], preferred_element_type=jnp.float32)
        active[column_rows, columns] = jax.nn.gelu(upward, approximate=True).astype(jnp.bfloat16)

    merge_pair()
    begin(up_pieces, 1)
    hop_send(0)
    begin(down_pieces, 1)
    ring_step(up_pieces, 1)
    ring_step(down_pieces, 1, (0,))
    hop_send(1)
    ring_step(up_pieces, 2)
    hop_send(2)
    for step in range(3, steps):
        ring_step(up_pieces, step)
    ring_step(down_pieces, 1, (1,))
    first_begin()
    ring_step(up_pieces, steps)
    ring_step(down_pieces, 2, (0,))
    first_forward()
    ring_step(down_pieces, 2, (1,))

    for k in range(slots):
        if k != local:
            remote(outgoing.at[k], incoming.at[k], slot_send.at[k], slot_recv.at[k], to_peer[k]).wait_recv()
        normed[pl.ds(k * BLOCK, BLOCK), :] = rms_scale(incoming[k].astype(jnp.float32), ng_ref[...]).astype(
            jnp.bfloat16
        )
    for piece in up_pieces:
        for xr in range(XHI):
            for dist in range(zs):
                arrived(piece, xr, dist, 1)

    ring_step(down_pieces, 3, (0,), up_part)
    second_begin()
    ring_step(down_pieces, 3, (1,), up_part)
    for step in range(4, steps):
        ring_step(down_pieces, step, between=up_part)
    for _ in range(up_parts // 2):
        up_part()
    second_forward()
    ring_step(down_pieces, steps, between=up_part)
    for _ in range(up_parts):
        up_part()
    for piece in down_pieces:
        for xr in range(XHI):
            for dist in range(zs):
                arrived(piece, xr, dist, 1)

    def give_back(k):
        send(remote(hidden.at[k], returned.at[k], back_send.at[k], back_recv.at[k], from_peer[k]))
        send(remote(estimate.at[k], estimate_back.at[k], value_send.at[k], value_recv.at[k], from_peer[k]))

    for first in range(0, slots, GROUP):
        downward = jnp.dot(
            active[pl.ds(first * BLOCK, GROUP * BLOCK), :], down_all[...], preferred_element_type=jnp.float32
        )
        for k in range(first, first + GROUP):
            part = downward[(k - first) * BLOCK : (k - first + 1) * BLOCK]
            final = rms_scale(incoming[k].astype(jnp.float32) + part, fg_ref[...])
            kept, kept_value = (returned, estimate_back) if k == local else (hidden, estimate)
            kept[k] = final.astype(jnp.bfloat16)
            value = jnp.tanh(jnp.sum(final * vw_ref[...], axis=-1, keepdims=True))
            kept_value[k] = jnp.transpose(jnp.broadcast_to(value, (BLOCK, BLOCK)))[0:8]
        for k in range(first, first + GROUP):
            if k != local:
                give_back(k)

    second_end()
    for k in range(slots):
        if k != local:
            remote(hidden.at[k], returned.at[k], back_send.at[k], back_recv.at[k], from_peer[k]).wait_recv()
            remote(
                estimate.at[k], estimate_back.at[k], value_send.at[k], value_recv.at[k], from_peer[k]
            ).wait_recv()
    for a in range(xs):
        for b in range(ys):
            ref = policy_rows(a, b, 1)
            remote(ref, ref, policy_core_send.at[a, b], policy_core_recv.at[a, b], sibling).wait_recv()

    count = count_ref[0]
    for b in range(bv_ref.shape[0]):
        block, value = returned[0], estimate_back[0]
        for k in range(1, slots):
            chosen = bv_ref[b] == to_peer[k][0]
            block = jnp.where(chosen, returned[k], block)
            value = jnp.where(chosen, estimate_back[k], value)
        own_hidden[pl.ds(b * BLOCK, BLOCK), :] = block
        games = b * BLOCK + lax.broadcasted_iota(jnp.int32, (1, BLOCK), 1)
        val_out[pl.ds(b, 1), :] = jnp.where(games < count, value[0:1], 0.0)

    games_here = policy_out.shape[0]
    live = lax.broadcasted_iota(jnp.int32, (games_here, 1), 0) < count

    def masked_logits(columns):
        logits = jnp.dot(own_hidden[...], policy_all[:, columns], preferred_element_type=jnp.float32)
        return jnp.where(live, logits, 0.0).astype(jnp.bfloat16)

    whole_tiles = moves // width

    def policy_tile_step(i, carry):
        columns = pl.ds(pl.multiple_of(i * width, width), width)
        policy_out[:, columns] = masked_logits(columns)
        return carry

    lax.fori_loop(0, whole_tiles, policy_tile_step, 0)
    rest = moves - whole_tiles * width
    if rest:
        policy_out[:, pl.ds(whole_tiles * width, rest)] = masked_logits(pl.ds(whole_tiles * width, width))[:, :rest]

    for copy in sent:
        copy.wait_send()


def local(
    positions,
    game_counts,
    block_variant,
    norm_gain,
    up_weight,
    down_weight,
    final_gain,
    value_weight,
    policy_weight,
):
    variants, members = lax.axis_size("variant"), lax.axis_size("mp")
    zs = members // (XHI * CORES)
    games_here, width = positions.shape
    blocks = block_variant.shape[0]
    up_rows, ffw = up_weight.shape[1:]
    down_rows = down_weight.shape[1]
    slots = variants
    vmem = pl.BlockSpec(memory_space=pltpu.VMEM)
    dma = pltpu.SemaphoreType.DMA
    policy_rows_here, moves = policy_weight.shape
    half_columns = -(-moves // (CORES * 128)) * 128
    tile_rows = 2 * CORES * policy_rows_here
    policy, value = pl.pallas_call(
        functools.partial(exchange_kernel, variants, members),
        out_shape=(
            jax.ShapeDtypeStruct((games_here, moves), jnp.bfloat16),
            jax.ShapeDtypeStruct((blocks, BLOCK), jnp.float32),
        ),
        in_specs=[pl.BlockSpec(memory_space=pltpu.SMEM)]
        + [vmem] * 6
        + [pl.BlockSpec(memory_space=pltpu.SMEM), vmem],
        out_specs=(vmem, vmem),
        scratch_shapes=[
            pltpu.VMEM((slots, BLOCK, width), jnp.bfloat16),
            pltpu.VMEM((slots, BLOCK, width), jnp.bfloat16),
            pltpu.VMEM((slots * BLOCK, width), jnp.bfloat16),
            pltpu.VMEM((slots * BLOCK, ffw), jnp.bfloat16),
            pltpu.VMEM((up_rows * members, ffw), jnp.bfloat16),
            pltpu.VMEM((down_rows * members, width), jnp.bfloat16),
            pltpu.VMEM((slots, BLOCK, width), jnp.bfloat16),
            pltpu.VMEM((slots, BLOCK, width), jnp.bfloat16),
            pltpu.VMEM((slots, 8, BLOCK), jnp.float32),
            pltpu.VMEM((slots, 8, BLOCK), jnp.float32),
            dma((4, XHI, zs, CORES)),
            dma((4, XHI, zs)),
            dma((4, XHI, zs)),
            dma((4, XHI, zs)),
            dma((4,)),
            dma((slots,)),
            dma((slots,)),
            dma((slots,)),
            dma((slots,)),
            dma((slots,)),
            dma((slots,)),
            pltpu.VMEM((games_here, width), jnp.bfloat16),
            pltpu.VMEM((tile_rows, CORES * half_columns), jnp.bfloat16),
            pltpu.VMEM((variants * members * policy_rows_here, CORES * half_columns), jnp.bfloat16),
            pltpu.VMEM((3, tile_rows, half_columns), jnp.bfloat16),
            dma((3,)),
            dma((3,)),
            dma((3,)),
            dma((3,)),
            dma((4,)),
            dma((4,)),
            dma((4, 3)),
            dma((4, 3)),
            dma((4, 4)),
            dma((4, 4)),
        ],
        compiler_params=pltpu.CompilerParams(
            collective_id=0, has_side_effects=True, vmem_limit_bytes=58 * 1024 * 1024
        ),
        cost_estimate=pl.CostEstimate(
            flops=4 * slots * BLOCK * width * ffw, bytes_accessed=4 * width * ffw, transcendentals=0
        ),
        name="exchange",
    )(
        block_variant,
        positions,
        up_weight[0],
        down_weight[0],
        norm_gain,
        final_gain,
        value_weight,
        game_counts,
        policy_weight,
    )
    return (policy, value.reshape(games_here))


def solution(mesh):
    in_specs = (
        P(("variant", "mp"), None),
        P(("variant", "mp")),
        P(("variant", "mp")),
        P("variant", None),
        P("variant", "mp", None),
        P("variant", "mp", None),
        P("variant", None),
        P("variant", None),
        P(("variant", "mp"), None),
    )
    out_specs = (P(("variant", "mp"), None), P(("variant", "mp")))
    return jax.shard_map(local, mesh=mesh, in_specs=in_specs, out_specs=out_specs, check_vma=False)
```

```python
import functools

import jax
import jax.numpy as jnp
from jax import lax
from jax.experimental import pallas as pl
from jax.experimental.pallas import tpu as pltpu
from jax.sharding import PartitionSpec as P

MESH = pl.DeviceIdType.MESH
BLOCK = 128
EPS = 1e-06
XLO, XHI, CORES = 2, 2, 2
GROUP = 2


def rms_scale(values, gain):
    mean_square = jnp.mean(values * values, axis=-1, keepdims=True)
    return values * lax.rsqrt(mean_square + EPS) * gain


def remote(src, dst, send_sem, recv_sem, device):
    return pltpu.make_async_remote_copy(
        src_ref=src, dst_ref=dst, send_sem=send_sem, recv_sem=recv_sem, device_id=device, device_id_type=MESH
    )


def exchange_kernel(
    variants,
    members,
    bv_ref,
    pos_ref,
    up_ref,
    down_ref,
    ng_ref,
    fg_ref,
    vw_ref,
    count_ref,
    rows_ref,
    policy_out,
    val_out,
    outgoing,
    incoming,
    normed,
    active,
    up_all,
    down_all,
    hidden,
    returned,
    estimate,
    estimate_back,
    ring_recv,
    plus_send,
    minus_send,
    core_send,
    half_send,
    slot_send,
    slot_recv,
    back_send,
    back_recv,
    value_send,
    value_recv,
    own_hidden,
    piece_ref,
    policy_all,
    pieces,
    piece_send,
    piece_recv,
    pair_send,
    pair_recv,
    first_send,
    first_recv,
    second_send,
    second_recv,
    policy_core_send,
    policy_core_recv,
):
    ys, zs = variants // XLO, members // (XHI * CORES)
    v, m = lax.axis_index("variant"), lax.axis_index("mp")
    y, xl = lax.div(v, XLO), lax.rem(v, XLO)
    xh, z, core = lax.div(m, zs * CORES), lax.rem(lax.div(m, CORES), zs), lax.rem(m, CORES)

    def member(xr, dz, cr):
        return (lax.rem(xh + xr, XHI) * zs + lax.rem(z + dz, zs)) * CORES + lax.rem(core + cr, CORES)

    def peer(dy, dx):
        return lax.rem(y + dy, ys) * XLO + lax.rem(xl + dx, XLO)

    z_plus, z_minus = (v, member(0, 1, 0)), (v, member(0, zs - 1, 0))
    sibling, half = (v, member(0, 0, 1)), (v, member(1, 0, 0))
    order = sorted(
        ((dy, dx) for dy in range(ys) for dx in range(XLO)), key=lambda r: (-min(r[0], ys - r[0]), -r[1])
    )
    to_peer = [(peer(dy, dx), m) for dy, dx in order]
    from_peer = [(peer(ys - dy, XLO - dx), m) for dy, dx in order]
    slots = len(order)
    local = slots - 1

    half_columns = policy_all.shape[1] // CORES
    tile_rows = piece_ref.shape[0]
    unit_rows = zs // 2 * tile_rows
    paired = z + 1 - 2 * lax.rem(z, 2) - z
    other_z = (v, member(0, zs + paired, 0))
    x = xh * XLO + xl
    xs = XHI * XLO

    def chip(cx, cy):
        cx, cy = lax.rem(cx, xs), lax.rem(cy, ys)
        return cy * XLO + lax.rem(cx, XLO), (lax.div(cx, XLO) * zs + z) * CORES + core

    def along(first, second):
        return x + first * (1 - core) + second * core, y + first * core + second * (1 - core)

    first_plus, first_minus = chip(*along(1, 0)), chip(*along(3, 0))
    second_plus, second_minus = chip(*along(0, 1)), chip(*along(0, 3))
    out_z = (v, member(0, zs - paired, 0))

    def policy_rows(a, b, cr, start=0, count=None):
        axis = lax.rem(core + cr, CORES)
        cx = lax.rem(x + (xs - a) * (1 - axis) + (xs - b) * axis, xs)
        cy = lax.rem(y + (ys - a) * axis + (ys - b) * (1 - axis), ys)
        group = (cy * XLO + lax.rem(cx, XLO)) * XHI + lax.div(cx, XLO)
        row = pl.multiple_of(group * unit_rows + start, tile_rows)
        column = pl.multiple_of(axis * half_columns, 128)
        return policy_all.at[pl.ds(row, unit_rows if count is None else count), pl.ds(column, half_columns)]

    def policy_tile(dz):
        return policy_rows(0, 0, 0, lax.div(lax.rem(z + dz, zs), 2) * tile_rows, tile_rows)

    barrier = pltpu.get_barrier_semaphore()
    greeted = [z_plus, z_minus, sibling, half, *to_peer[:local], (peer(0, 1), member(1, 0, 0))]
    for device in greeted:
        pl.semaphore_signal(barrier, inc=1, device_id=device, device_id_type=MESH)

    shards, wholes = (up_ref, down_ref), (up_all, down_all)

    up_pieces, down_pieces = (0, 1), (2, 3)

    def rows(piece, xr, dist, cr):
        kind, part = divmod(piece, 2)
        depth = shards[kind].shape[0]
        owner = member(xr, zs - dist, cr)
        start = pl.multiple_of(owner * depth + part * (depth // 2), depth // 2)
        return wholes[kind].at[pl.ds(start, depth // 2)]

    def own(piece):
        kind, part = divmod(piece, 2)
        depth = shards[kind].shape[0]
        return shards[kind].at[pl.ds(part * (depth // 2), depth // 2)]

    def source(piece, xr, dist):
        return own(piece) if (xr, dist) == (0, 0) else rows(piece, xr, dist, 0)

    sent = []

    def send(copy):
        copy.start()
        sent.append(copy)

    def send_half(piece):
        send(remote(own(piece), rows(piece, 0, 0, 0), half_send.at[piece], ring_recv.at[piece, 1, 0, 0], half))

    def ring_send(piece, xr, dist, sems, dist_there, cr_there, device):
        send(
            remote(
                source(piece, xr, dist),
                rows(piece, xr, dist, 0),
                sems.at[piece, xr, dist],
                ring_recv.at[piece, xr, dist_there, cr_there],
                device,
            )
        )

    def send_plus(piece, xr, dist):
        ring_send(piece, xr, dist, plus_send, dist + 1, 0, z_plus)

    def send_minus(piece, xr, dist):
        ring_send(piece, xr, dist, minus_send, (dist - 1) % zs, 0, z_minus)

    def send_core(piece, xr, dist):
        ring_send(piece, xr, dist, core_send, dist, 1, sibling)

    def arrived(piece, xr, dist, cr):
        ref = rows(piece, xr, dist, cr)
        remote(ref, ref, core_send.at[piece, xr, dist], ring_recv.at[piece, xr, dist, cr], sibling).wait_recv()

    plus = (zs // 2, zs - 1 - zs // 2)
    minus = (zs - 1 - zs // 2, zs // 2)
    steps = zs // 2

    def begin(pieces_here, xr):
        for piece in pieces_here:
            if xr:
                arrived(piece, xr, 0, 0)
            send_plus(piece, xr, 0)
            send_minus(piece, xr, 0)
        for piece in pieces_here:
            send_core(piece, xr, 0)

    def ring_step(pieces_here, step, halves=(0, 1), between=None):
        kind = pieces_here[0] // 2
        for xr in halves:
            for piece in pieces_here:
                if step <= plus[kind]:
                    arrived(piece, xr, step, 0)
                    if step < plus[kind]:
                        send_plus(piece, xr, step)
                    send_core(piece, xr, step)
                if step <= minus[kind]:
                    arrived(piece, xr, zs - step, 0)
                    if step < minus[kind]:
                        send_minus(piece, xr, zs - step)
                    send_core(piece, xr, zs - step)
                if between is not None:
                    between()

    own_columns = pl.ds(pl.multiple_of(core * half_columns, 128), half_columns)
    sibling_columns = pl.ds(pl.multiple_of((1 - core) * half_columns, 128), half_columns)

    def piece_copy(i):
        source_ref = piece_ref.at[:, sibling_columns] if i == 0 else pieces.at[2]
        return remote(source_ref, pieces.at[i], piece_send.at[i], piece_recv.at[i], (sibling, other_z)[i])

    def merge_chip():
        piece_copy(0).wait_recv()
        mine = piece_ref[:, own_columns].astype(jnp.float32)
        pieces[2] = (mine + pieces[0].astype(jnp.float32)).astype(jnp.bfloat16)

    def merge_pair():
        piece_copy(1).wait_recv()
        total = pieces[2].astype(jnp.float32) + pieces[1].astype(jnp.float32)
        policy_tile(0)[...] = total.astype(jnp.bfloat16)

    hop_sent = (0, zs - paired, 2 * zs + 2 * paired)
    hop_got = (zs - paired, 2 * zs + 2 * paired, 3 * zs - 3 * paired)

    def hop_copy(i, dz):
        ref = policy_tile(dz)
        return remote(ref, ref, pair_send.at[i], pair_recv.at[i], (out_z, other_z, out_z)[i])

    def hop_send(i):
        if i:
            hop_copy(i - 1, hop_got[i - 1]).wait_recv()
        send(hop_copy(i, hop_sent[i]))

    def policy_to_core(a, b):
        ref = policy_rows(a, b, 0)
        send(remote(ref, ref, policy_core_send.at[a, b], policy_core_recv.at[a, b], sibling))

    part_unit = unit_rows // 2

    def first_copy(i, a):
        ref = policy_rows(a, 0, 0) if i < 2 else policy_rows(a, 0, 0, (i - 2) * part_unit, part_unit)
        return remote(ref, ref, first_send.at[i], first_recv.at[i], (first_plus, first_minus)[i % 2])

    def first_begin():
        hop_copy(2, hop_got[2]).wait_recv()
        send(first_copy(0, 0))
        send(first_copy(1, 0))
        second_send_rows(0)
        policy_to_core(0, 0)

    def first_forward():
        for i, a in ((0, 1), (1, 3)):
            first_copy(i, a).wait_recv()
            send(first_copy(2 + i, a))
            second_send_rows(a)
            policy_to_core(a, 0)

    def second_copy(a, i, b):
        ref = policy_rows(a, b, 0)
        device = second_plus if i == 0 or (i == 2 and a < 2) else second_minus
        return remote(ref, ref, second_send.at[a, i], second_recv.at[a, i], device)

    def second_begin():
        for i in (2, 3):
            first_copy(i, 2).wait_recv()
        second_send_rows(2)
        policy_to_core(2, 0)

    def second_send_rows(a):
        send(second_copy(a, 0, 0))
        send(second_copy(a, 1, 0))

    def second_forward(groups):
        for a in groups:
            for i, b in ((0, 1), (1, 3)):
                second_copy(a, i, b).wait_recv()
                if (i == 0) == (a < 2):
                    send(second_copy(a, 2, b))
                policy_to_core(a, b)

    def second_end():
        for a in range(xs):
            second_copy(a, 2, 2).wait_recv()
            policy_to_core(a, 2)

    def fill(k):
        wanted = to_peer[k][0]
        block = pos_ref[0:BLOCK, :]
        for b in range(1, bv_ref.shape[0]):
            block = jnp.where(bv_ref[b] == wanted, pos_ref[b * BLOCK : (b + 1) * BLOCK, :], block)
        if k == local:
            incoming[k] = block
        else:
            outgoing[k] = block

    def dispatch(k):
        send(remote(outgoing.at[k], incoming.at[k], slot_send.at[k], slot_recv.at[k], to_peer[k]))

    rows_here, moves = rows_ref.shape
    place = lax.rem(m, tile_rows // rows_here) * rows_here
    spread = lax.broadcasted_iota(jnp.int32, (tile_rows, rows_here), 0) == place + lax.broadcasted_iota(
        jnp.int32, (tile_rows, rows_here), 1
    )
    piece_ref[...] = jnp.zeros(piece_ref.shape, jnp.bfloat16)
    piece_ref[:, :moves] = jnp.dot(
        spread.astype(jnp.bfloat16), rows_ref[...], preferred_element_type=jnp.float32
    ).astype(jnp.bfloat16)
    for k in range(slots):
        fill(k)

    pl.semaphore_wait(barrier, len(greeted))
    send(piece_copy(0))
    for piece in (*up_pieces, *down_pieces):
        send_half(piece)
    begin(up_pieces, 0)
    for k in range(local):
        dispatch(k)
    merge_chip()

    for kind in range(2):
        depth = shards[kind].shape[0]
        wholes[kind][pl.ds(pl.multiple_of(m * depth, depth), depth), :] = shards[kind][...]

    send(piece_copy(1))
    begin(down_pieces, 0)

    total_rows = normed.shape[0]
    part_rows = total_rows // 2
    width = 256
    up_parts = 2 * (up_all.shape[1] // width)
    made = []

    def up_part():
        index = len(made)
        if index >= up_parts:
            return
        made.append(index)
        column_rows = pl.ds(index % 2 * part_rows, part_rows)
        columns = pl.ds(index // 2 * width, width)
        upward = jnp.dot(normed[column_rows, :], up_all[:, columns], preferred_element_type=jnp.float32)
        active[column_rows, columns] = jax.nn.gelu(upward, approximate=True).astype(jnp.bfloat16)

    merge_pair()
    begin(up_pieces, 1)
    hop_send(0)
    begin(down_pieces, 1)
    ring_step(up_pieces, 1)
    ring_step(down_pieces, 1, (0,))
    hop_send(1)
    ring_step(up_pieces, 2)
    hop_send(2)
    for step in range(3, steps):
        ring_step(up_pieces, step)
    ring_step(down_pieces, 1, (1,))
    first_begin()
    ring_step(up_pieces, steps)
    ring_step(down_pieces, 2, (0,))
    first_forward()
    ring_step(down_pieces, 2, (1,))

    for k in range(slots):
        if k != local:
            remote(outgoing.at[k], incoming.at[k], slot_send.at[k], slot_recv.at[k], to_peer[k]).wait_recv()
        normed[pl.ds(k * BLOCK, BLOCK), :] = rms_scale(incoming[k].astype(jnp.float32), ng_ref[...]).astype(
            jnp.bfloat16
        )
    for piece in up_pieces:
        for xr in range(XHI):
            for dist in range(zs):
                arrived(piece, xr, dist, 1)

    second_begin()
    for step in range(3, steps):
        ring_step(down_pieces, step, between=up_part)
    for _ in range(up_parts // 2):
        up_part()
    second_forward((0, 1, 3))
    ring_step(down_pieces, steps, between=up_part)
    second_forward((2,))
    for _ in range(up_parts):
        up_part()
    for piece in down_pieces:
        for xr in range(XHI):
            for dist in range(zs):
                arrived(piece, xr, dist, 1)

    def give_back(k):
        send(remote(hidden.at[k], returned.at[k], back_send.at[k], back_recv.at[k], from_peer[k]))
        send(remote(estimate.at[k], estimate_back.at[k], value_send.at[k], value_recv.at[k], from_peer[k]))

    for first in range(0, slots, GROUP):
        downward = jnp.dot(
            active[pl.ds(first * BLOCK, GROUP * BLOCK), :], down_all[...], preferred_element_type=jnp.float32
        )
        for k in range(first, first + GROUP):
            part = downward[(k - first) * BLOCK : (k - first + 1) * BLOCK]
            final = rms_scale(incoming[k].astype(jnp.float32) + part, fg_ref[...])
            kept, kept_value = (returned, estimate_back) if k == local else (hidden, estimate)
            kept[k] = final.astype(jnp.bfloat16)
            value = jnp.tanh(jnp.sum(final * vw_ref[...], axis=-1, keepdims=True))
            kept_value[k] = jnp.transpose(jnp.broadcast_to(value, (BLOCK, BLOCK)))[0:8]
        for k in range(first, first + GROUP):
            if k != local:
                give_back(k)

    second_end()
    for k in range(slots):
        if k != local:
            remote(hidden.at[k], returned.at[k], back_send.at[k], back_recv.at[k], from_peer[k]).wait_recv()
            remote(
                estimate.at[k], estimate_back.at[k], value_send.at[k], value_recv.at[k], from_peer[k]
            ).wait_recv()
    for a in range(xs):
        for b in range(ys):
            ref = policy_rows(a, b, 1)
            remote(ref, ref, policy_core_send.at[a, b], policy_core_recv.at[a, b], sibling).wait_recv()

    count = count_ref[0]
    for b in range(bv_ref.shape[0]):
        block, value = returned[0], estimate_back[0]
        for k in range(1, slots):
            chosen = bv_ref[b] == to_peer[k][0]
            block = jnp.where(chosen, returned[k], block)
            value = jnp.where(chosen, estimate_back[k], value)
        own_hidden[pl.ds(b * BLOCK, BLOCK), :] = block
        games = b * BLOCK + lax.broadcasted_iota(jnp.int32, (1, BLOCK), 1)
        val_out[pl.ds(b, 1), :] = jnp.where(games < count, value[0:1], 0.0)

    games_here = policy_out.shape[0]
    live = lax.broadcasted_iota(jnp.int32, (games_here, 1), 0) < count

    def masked_logits(columns):
        logits = jnp.dot(own_hidden[...], policy_all[:, columns], preferred_element_type=jnp.float32)
        return jnp.where(live, logits, 0.0).astype(jnp.bfloat16)

    whole_tiles = moves // width

    def policy_tile_step(i, carry):
        columns = pl.ds(pl.multiple_of(i * width, width), width)
        policy_out[:, columns] = masked_logits(columns)
        return carry

    lax.fori_loop(0, whole_tiles, policy_tile_step, 0)
    rest = moves - whole_tiles * width
    if rest:
        policy_out[:, pl.ds(whole_tiles * width, rest)] = masked_logits(pl.ds(whole_tiles * width, width))[:, :rest]

    for copy in sent:
        copy.wait_send()


def local(
    positions,
    game_counts,
    block_variant,
    norm_gain,
    up_weight,
    down_weight,
    final_gain,
    value_weight,
    policy_weight,
):
    variants, members = lax.axis_size("variant"), lax.axis_size("mp")
    zs = members // (XHI * CORES)
    games_here, width = positions.shape
    blocks = block_variant.shape[0]
    up_rows, ffw = up_weight.shape[1:]
    down_rows = down_weight.shape[1]
    slots = variants
    vmem = pl.BlockSpec(memory_space=pltpu.VMEM)
    dma = pltpu.SemaphoreType.DMA
    policy_rows_here, moves = policy_weight.shape
    half_columns = -(-moves // (CORES * 128)) * 128
    tile_rows = 2 * CORES * policy_rows_here
    policy, value = pl.pallas_call(
        functools.partial(exchange_kernel, variants, members),
        out_shape=(
            jax.ShapeDtypeStruct((games_here, moves), jnp.bfloat16),
            jax.ShapeDtypeStruct((blocks, BLOCK), jnp.float32),
        ),
        in_specs=[pl.BlockSpec(memory_space=pltpu.SMEM)]
        + [vmem] * 6
        + [pl.BlockSpec(memory_space=pltpu.SMEM), vmem],
        out_specs=(vmem, vmem),
        scratch_shapes=[
            pltpu.VMEM((slots, BLOCK, width), jnp.bfloat16),
            pltpu.VMEM((slots, BLOCK, width), jnp.bfloat16),
            pltpu.VMEM((slots * BLOCK, width), jnp.bfloat16),
            pltpu.VMEM((slots * BLOCK, ffw), jnp.bfloat16),
            pltpu.VMEM((up_rows * members, ffw), jnp.bfloat16),
            pltpu.VMEM((down_rows * members, width), jnp.bfloat16),
            pltpu.VMEM((slots, BLOCK, width), jnp.bfloat16),
            pltpu.VMEM((slots, BLOCK, width), jnp.bfloat16),
            pltpu.VMEM((slots, 8, BLOCK), jnp.float32),
            pltpu.VMEM((slots, 8, BLOCK), jnp.float32),
            dma((4, XHI, zs, CORES)),
            dma((4, XHI, zs)),
            dma((4, XHI, zs)),
            dma((4, XHI, zs)),
            dma((4,)),
            dma((slots,)),
            dma((slots,)),
            dma((slots,)),
            dma((slots,)),
            dma((slots,)),
            dma((slots,)),
            pltpu.VMEM((games_here, width), jnp.bfloat16),
            pltpu.VMEM((tile_rows, CORES * half_columns), jnp.bfloat16),
            pltpu.VMEM((variants * members * policy_rows_here, CORES * half_columns), jnp.bfloat16),
            pltpu.VMEM((3, tile_rows, half_columns), jnp.bfloat16),
            dma((3,)),
            dma((3,)),
            dma((3,)),
            dma((3,)),
            dma((4,)),
            dma((4,)),
            dma((4, 3)),
            dma((4, 3)),
            dma((4, 4)),
            dma((4, 4)),
        ],
        compiler_params=pltpu.CompilerParams(
            collective_id=0, has_side_effects=True, vmem_limit_bytes=58 * 1024 * 1024
        ),
        cost_estimate=pl.CostEstimate(
            flops=4 * slots * BLOCK * width * ffw, bytes_accessed=4 * width * ffw, transcendentals=0
        ),
        name="exchange",
    )(
        block_variant,
        positions,
        up_weight[0],
        down_weight[0],
        norm_gain,
        final_gain,
        value_weight,
        game_counts,
        policy_weight,
    )
    return (policy, value.reshape(games_here))


def solution(mesh):
    in_specs = (
        P(("variant", "mp"), None),
        P(("variant", "mp")),
        P(("variant", "mp")),
        P("variant", None),
        P("variant", "mp", None),
        P("variant", "mp", None),
        P("variant", None),
        P("variant", None),
        P(("variant", "mp"), None),
    )
    out_specs = (P(("variant", "mp"), None), P(("variant", "mp")))
    return jax.shard_map(local, mesh=mesh, in_specs=in_specs, out_specs=out_specs, check_vma=False)
```
